256 devices in a mesh: path: 16 (over z, core), tm: 16 (over y, x).
Axes of the slice: x: 4, y: 4, z: 8, core: 2. Of those that a mesh axis runs over, the one named last changes fastest.
Arguments:
- shock_rate: float32 [256, 262144], P('tm', 'path'), may hold values from -6 to 6
- shock_fx: float32 [4, 256, 262144], P(None, 'tm', 'path'), may hold values from -6 to 6
- fx_vol: float32 [4], replicated, may hold values from 0.1 to 0.4
- fx_corr: float32 [4], replicated, may hold values from -0.8 to 0.8
- hazard_scale: float32 [32], replicated, may hold values from 0.03 to 3
- counterparty: int32 [512], replicated, may hold values from 0 to 31
- currency: int32 [512], replicated, may hold values from 0 to 3
- maturity: int32 [512], replicated, may hold values from 1 to 256
- notional: float32 [512], replicated, may hold values from -8 to 8
- strike: float32 [512], replicated, may hold values from 0.7 to 1.3
Outputs:
- profile: float32 [256, 32], P('tm')
- cva: float32 [32], replicated
The draws below stay inside these ranges and needn't reach their ends.
All inputs are finite; a program needn't handle non-finite values.
Results may differ from the reference program's by a relative error of at most 0.000061.
Values sent between devices are 32-bit elements; how exact they have to be, the bound alone decides.
A program may use at most 64 MiB of HBM per device.

```python
import math
import jax
import jax.numpy as jnp
from jax import lax

NCCY = 4
NCP = 32
NTRADE = 512
DATES = 256
PATHS = 262144


def plant(drawn, key, least, largest):
    dims = drawn.shape
    place = [jax.random.randint(jax.random.fold_in(key, axis), (), 0, dims[axis]) for axis in range(len(dims))]
    drawn = drawn.at[tuple(place)].set(least)
    longest = dims.index(max(dims))
    place[longest] = (place[longest] + 1) % dims[longest]
    return drawn.at[tuple(place)].set(largest)


def levels(own_key, shape, shards, low, largest):
    factor_of, own = 1.0, jax.random.fold_in(own_key, 6)
    for position, parts in shards:
        steps = jnp.exp(jax.random.uniform(jax.random.fold_in(own, position), (parts,), jnp.float32, low / len(shards), largest / len(shards)))
        factor_of = factor_of * jnp.repeat(steps, shape[position] // parts).reshape([-1 if axis == position else 1 for axis in range(len(shape))])
    return factor_of


def normal_values(stream_key, extent, spread, reach, shards=(), held_as=jnp.bfloat16):
    factor_of = levels(stream_key, extent, shards, -0.22, 0.18) if shards else 1.0
    result = jax.random.normal(stream_key, extent, jnp.float32) * spread * factor_of
    return jnp.minimum(jnp.maximum(result, -reach), reach).astype(held_as)


def setup_inputs(seed: int = 0) -> dict:
    keys = jax.random.split(jax.random.key(seed), 11)
    shock_rate = normal_values(keys[0], (DATES, PATHS), 1.0, 6.0, ((0, 16), (1, 16)), jnp.float32)
    shock_fx = normal_values(keys[1], (NCCY, DATES, PATHS), 1.0, 6.0, ((1, 16), (2, 16)), jnp.float32)
    fx_vol = jnp.clip(jnp.exp(jax.random.uniform(keys[2], (NCCY,), jnp.float32, math.log(0.1), math.log(0.4))), 0.1, 0.4)
    fx_corr = jnp.clip(jax.random.uniform(keys[3], (NCCY,), jnp.float32, -0.8, 0.8), -0.8, 0.8)
    hazard_scale = jnp.clip(jnp.exp(jax.random.uniform(keys[4], (NCP,), jnp.float32, math.log(0.03), math.log(3.0))), 0.03, 3.0)
    counterparty = plant(jax.random.randint(keys[5], (NTRADE,), 0, NCP), jax.random.fold_in(keys[5], 1), 0, NCP - 1).astype(jnp.int32)
    currency = plant(jax.random.randint(keys[6], (NTRADE,), 0, NCCY), jax.random.fold_in(keys[6], 1), 0, NCCY - 1).astype(jnp.int32)
    maturity = plant(jax.random.randint(keys[7], (NTRADE,), 1, DATES + 1), jax.random.fold_in(keys[7], 1), 1, DATES).astype(jnp.int32)
    notional = normal_values(keys[8], (NTRADE,), 2.0, 8.0, (), jnp.float32)
    strike = jnp.clip(jax.random.uniform(keys[9], (NTRADE,), jnp.float32, 0.7, 1.3), 0.7, 1.3)
    return {"shock_rate": shock_rate, "shock_fx": shock_fx, "fx_vol": fx_vol, "fx_corr": fx_corr, "hazard_scale": hazard_scale, "counterparty": counterparty, "currency": currency, "maturity": maturity, "notional": notional, "strike": strike}


HORIZON = 5.0
RATE_DOM = 0.03
RATE_FOR = 0.01
LOSS_SHARE = 0.6
RATE_SHIFT = 1.5
HIGHEST_PREC = lax.Precision.HIGHEST

def trade_tables(date_rows, counterparty, currency, maturity, notional, strike, cp_count, ccy_count, date_step):
    expiry = maturity.astype(jnp.int32)
    is_alive = (date_rows[:, None] < expiry[None, :]).astype(jnp.float32)
    time_left = (expiry[None, :] - date_rows[:, None]).astype(jnp.float32) * date_step
    weight_for = is_alive * notional[None, :] * jnp.exp(-RATE_FOR * time_left)
    weight_dom = is_alive * (notional * strike)[None, :] * jnp.exp(-RATE_DOM * time_left)
    member = (counterparty.astype(jnp.int32)[None, :] == jnp.arange(cp_count, dtype=jnp.int32)[:, None]).astype(jnp.float32)
    currency_onehot = (currency.astype(jnp.int32)[None, :] == jnp.arange(ccy_count, dtype=jnp.int32)[:, None]).astype(jnp.float32)
    fwd_table = jnp.einsum('ck,tk,jk->tcj', member, weight_for, currency_onehot, precision=HIGHEST_PREC)
    dom_table = jnp.einsum('ck,tk->tc', member, weight_dom, precision=HIGHEST_PREC)
    return (fwd_table, dom_table)

def weigh_block(block_item, hazard_scale):
    fwd_table, dom_table, spot, hazard_prev, hazard_cur = block_item
    netted = jnp.einsum('tcj,tjp->tcp', fwd_table, spot, precision=HIGHEST_PREC) - dom_table[:, :, None]
    exposure = jnp.maximum(netted, 0.0)
    scale_row = hazard_scale[None, :, None]
    density = jnp.exp(-scale_row * hazard_prev[:, None, :]) - jnp.exp(-scale_row * hazard_cur[:, None, :])
    return lax.optimization_barrier(jnp.sum(exposure * density, axis=2))

def weigh_dates(fwd_table, dom_table, spot, hazard_prev, hazard_cur, hazard_scale):
    date_count, path_count = hazard_cur.shape
    cp_count = dom_table.shape[1]
    ccy_count = spot.shape[1]
    block_dates = math.gcd(date_count, max(1, 32768 // path_count))
    groups = date_count // block_dates
    blocks = (fwd_table.reshape(groups, block_dates, cp_count, ccy_count), dom_table.reshape(groups, block_dates, cp_count), spot.reshape(groups, block_dates, ccy_count, path_count), hazard_prev.reshape(groups, block_dates, path_count), hazard_cur.reshape(groups, block_dates, path_count))
    weighed = lax.map(lambda block_item: weigh_block(block_item, hazard_scale), blocks)
    return weighed.reshape(date_count, cp_count)

def reference(shock_rate, shock_fx, fx_vol, fx_corr, hazard_scale, counterparty, currency, maturity, notional, strike):
    date_step = HORIZON / DATES
    decay_rate = math.exp(-2.0 / DATES)
    noise_scale = math.sqrt(1.0 - decay_rate * decay_rate)
    mix_weight = jnp.sqrt(1.0 - fx_corr * fx_corr)
    fx_shock = fx_vol * math.sqrt(date_step)
    fx_drift = 0.5 * fx_vol * fx_vol * date_step

    def advance(state, shocks):
        rate_state, hazard, log_spot = state
        rate_shock, other_shock = shocks
        rate_state = decay_rate * rate_state + noise_scale * rate_shock
        shifted = rate_state + RATE_SHIFT
        hazard_next = hazard + date_step * (0.1 + 0.5 * shifted * shifted)
        mixed = fx_corr[:, None] * rate_shock[None, :] + mix_weight[:, None] * other_shock
        log_spot = log_spot + (fx_shock[:, None] * mixed - fx_drift[:, None])
        return ((rate_state, hazard_next, log_spot), (hazard, hazard_next, jnp.exp(log_spot)))
    start = (jnp.zeros((PATHS,), jnp.float32), jnp.zeros((PATHS,), jnp.float32), jnp.zeros((NCCY, PATHS), jnp.float32))
    ignored, outputs = lax.scan(advance, start, (shock_rate, jnp.moveaxis(shock_fx, 1, 0)))
    hazard_prev, hazard_cur, spot = outputs
    date_rows = jnp.arange(DATES, dtype=jnp.int32)
    fwd_table, dom_table = trade_tables(date_rows, counterparty, currency, maturity, notional, strike, NCP, NCCY, date_step)
    weighed = weigh_dates(fwd_table, dom_table, spot, hazard_prev, hazard_cur, hazard_scale)
    profile = weighed / (PATHS * date_step)
    discount = jnp.exp(-RATE_DOM * date_step * (date_rows.astype(jnp.float32) + 1.0))
    cva = LOSS_SHARE * date_step * lax.optimization_barrier(jnp.sum(discount[:, None] * profile, axis=0))
    return (profile, cva)
```

```python
import functools
import math

import jax
import jax.numpy as jnp
from jax import lax
from jax.experimental import pallas as pl
from jax.experimental.pallas import tpu as pltpu
from jax.sharding import PartitionSpec as P

HORIZON = 5.0
RATE_DOM = 0.03
RATE_FOR = 0.01
LOSS_SHARE = 0.6
RATE_SHIFT = 1.5
LOG2E = 1.4426950408889634

CHUNKS = 4
GROUP = 2048
MESH = pl.DeviceIdType.MESH
F32 = jnp.float32
BF16 = jnp.bfloat16


def split3(x):
    high = x.astype(BF16)
    rest = x - high.astype(F32)
    mid = rest.astype(BF16)
    low = (rest - mid.astype(F32)).astype(BF16)
    return high, mid, low


def iota(shape, dim):
    return lax.broadcasted_iota(jnp.int32, shape, dim)


def ones_where(mask):
    return jnp.where(mask, 1.0, 0.0)


def kernel(
    geometry,
    rate_hbm, fx_hbm, vol_s, corr_s, scale_s, cp_ref, ccy_ref, mat_ref, notl_ref, strike_ref,
    prof_out, cva_out,
    xr, xf, log_ref, ab_ref, sum_ref, rcv_ref, pre_ref, st_ref,
    m1_ref, m2_ref, lhs_ref, wf_ref, wd_ref, ns_ref, net_ref, haz_ref, acc_ref,
    part_ref, parts_rcv, cpart_ref, cparts_rcv,
    in_sem, s1_send, s1_recv, s2_send, s2_recv, t_send, t_recv,
):
    n_tm, n_path, paths, dates, cps, ccys, total_dates, total_paths = geometry
    dt = HORIZON / total_dates
    decay = math.exp(-2.0 / total_dates)
    noise = math.sqrt(1.0 - decay * decay)
    width = paths // (CHUNKS * n_tm)
    tiles = CHUNKS * n_tm
    chunk_paths = n_tm * width
    group = min(GROUP, chunk_paths)
    me = lax.axis_index("tm")
    my_path = lax.axis_index("path")

    def load_copies(k):
        lanes = pl.ds(k * chunk_paths, chunk_paths)
        return (
            pltpu.make_async_copy(rate_hbm.at[:, lanes], xr.at[:, lanes], in_sem.at[0, k]),
            pltpu.make_async_copy(fx_hbm.at[:, :, lanes], xf.at[:, :, lanes], in_sem.at[1, k]),
        )

    for k in range(CHUNKS):
        for copy in load_copies(k):
            copy.start()

    barrier = pltpu.get_barrier_semaphore()

    @pl.loop(1, n_tm)
    def _(i):
        pl.semaphore_signal(barrier, inc=1, device_id={"tm": lax.rem(me + i, n_tm)}, device_id_type=MESH)

    @pl.loop(1, n_path)
    def _(i):
        pl.semaphore_signal(
            barrier, inc=1, device_id={"path": lax.rem(my_path + i, n_path)}, device_id_type=MESH
        )

    r, c = iota((96, 256), 0), iota((96, 256), 1)
    s = c - jnp.where(c >= 80, 80, 0) - jnp.where(c >= 160, 80, 0)
    in_ccy, in_date = (s >> 4) - 1, s & 15
    last = jnp.full_like(r, 15)
    out_ccy = jnp.where(r < 64, (r & 31) >> 3, jnp.where((r < 80) | (r == 80), -1, jnp.where(r < 85, r - 81, 9)))
    out_date = jnp.where(r < 64, ((r >> 5) << 3) + (r & 7), jnp.where(r < 80, r - 64, last))
    m1_ref[...] = ones_where((c < 240) & (in_ccy == out_ccy) & (in_date <= out_date)).astype(BF16)
    r, c = iota((48, 128), 0), iota((48, 128), 1)
    s = c & 31
    in_kind, in_date = s >> 4, s & 15
    out_kind = jnp.where(r < 32, r >> 4, jnp.where(r == 37, 0, jnp.where(r == 38, 1, 9)))
    out_date = jnp.where(r < 32, r & 15, jnp.full_like(r, 15))
    m2_ref[...] = ones_where((c < 96) & (in_kind == out_kind) & (in_date <= out_date)).astype(BF16)

    def vec(ref, j):
        return jnp.full((1, 128), ref[j], F32)

    def wide(v, n):
        return jnp.broadcast_to(v[:, :1], (v.shape[0], n))

    c_rate, c_own, c_drift = [], [], []
    for j in range(ccys):
        vol, corr = vec(vol_s, j), vec(corr_s, j)
        c_rate.append(wide(vol * math.sqrt(dt) * corr, group))
        c_own.append(wide(vol * math.sqrt(dt) * jnp.sqrt(1.0 - corr * corr), group))
        c_drift.append(wide(0.5 * vol * vol * dt, group))

    def date_col(n):
        return iota((dates, n), 0).astype(F32)

    log_decay = -2.0 / total_dates

    def walk(first, k, u):
        lanes = pl.ds(pl.multiple_of(first, group), group)
        rate = xr[:, lanes]
        rows = [rate * (noise * jnp.exp(-log_decay * date_col(group)))]
        for j in range(ccys):
            rows.append((c_rate[j] * rate + c_own[j] * xf[j, :, lanes]) - c_drift[j])
        high, mid, low = split3(jnp.concatenate(rows, axis=0))
        right = jnp.concatenate([high, mid, low, jnp.zeros((16, group), BF16)], axis=0)
        out = jnp.dot(m1_ref[...], right, preferred_element_type=F32)
        power = jnp.exp(log_decay * date_col(group))
        shifted = out[64:80] * power + RATE_SHIFT
        cost = dt * (0.1 + 0.5 * shifted * shifted)
        slope = (dt * decay) * power * shifted
        high, mid, low = split3(jnp.concatenate([cost, slope], axis=0))
        right = jnp.concatenate([high, mid, low, jnp.zeros((32, group), BF16)], axis=0)
        out2 = jnp.dot(m2_ref[...], right, preferred_element_type=F32)
        row = iota((8, group), 0)
        ends = jnp.where(row == 0, decay ** (dates - 1), 1.0) * out[80:88] + out2[32:40]
        tile0 = first // width
        for q in range(group // width):
            part = slice(q * width, (q + 1) * width)
            log_ref[tile0 + q] = out[:64, part]
            ab_ref[tile0 + q] = out2[:32, part]
            sum_ref[tile0 + q] = ends[:, part]

    def send1(k, i):
        owner = lax.rem(me + i, n_tm)
        return pltpu.make_async_remote_copy(
            src_ref=sum_ref.at[k * n_tm + owner],
            dst_ref=rcv_ref.at[k, me],
            send_sem=s1_send.at[k],
            recv_sem=s1_recv.at[k],
            device_id={"tm": owner},
            device_id_type=MESH,
        )

    def send2(k, i):
        block = lax.rem(me + i, n_tm)
        return pltpu.make_async_remote_copy(
            src_ref=pre_ref.at[k, block],
            dst_ref=st_ref.at[k * n_tm + me],
            send_sem=s2_send.at[k],
            recv_sem=s2_recv.at[k],
            device_id={"tm": block},
            device_id_type=MESH,
        )

    def all_of(send, recv, k):
        return pltpu.make_async_remote_copy(
            src_ref=rcv_ref.at[k, pl.ds(0, n_tm - 1)],
            dst_ref=rcv_ref.at[k, pl.ds(0, n_tm - 1)],
            send_sem=send.at[k],
            recv_sem=recv.at[k],
            device_id={"tm": me},
            device_id_type=MESH,
        )

    for k in range(CHUNKS):
        for copy in load_copies(k):
            copy.wait()
        for u in range(chunk_paths // group):
            walk(k * chunk_paths + u * group, k, u)
        if k == 0:
            pl.semaphore_wait(barrier, n_tm - 1 + n_path - 1)

        @pl.loop(1, n_tm)
        def _(i):
            send1(k, i).start()

    cp, ccy, mat = cp_ref[...], ccy_ref[...], mat_ref[...]
    trades = cp.shape[1]
    date = iota((dates, trades), 0) + me * dates
    alive = date < mat
    left = (mat - date).astype(F32) * dt
    notl = notl_ref[...]
    wf_ref[...] = jnp.where(alive, notl * jnp.exp(-RATE_FOR * left), 0.0)
    wd_ref[...] = jnp.where(alive, -(notl * strike_ref[...]) * jnp.exp(-RATE_DOM * left), 0.0)
    member = cp == iota((cps, trades), 0)
    col = iota((256, trades), 0)
    pick = jnp.concatenate(
        [
            ones_where((col < 192) & (ccy == ((col & 31) >> 3))).astype(BF16),
            ones_where((col >= 192) & (col < 195)).astype(BF16),
        ],
        axis=1,
    )
    r, c = iota((256, 256), 0), iota((256, 256), 1)
    keep = (c >= 192) | ((r >> 5) == (c & 7))
    part = c >> 5
    is_high = (part == 0) | (part == 3) | (part == 5) | (c == 192)
    is_mid = (part == 1) | (part == 4) | (c == 193)
    for half in range(2):
        blocks = []
        for t in range(half * 8, half * 8 + 8):
            blocks.append(
                jnp.concatenate(
                    [
                        jnp.where(member, wf_ref[t : t + 1], 0.0),
                        jnp.where(member, wd_ref[t : t + 1], 0.0),
                    ],
                    axis=1,
                )
            )
        table = jnp.zeros((256, 256), F32)
        for piece in split3(jnp.concatenate(blocks, axis=0)):
            table = table + lax.dot_general(
                piece, pick, (((1,), (1,)), ((), ())), preferred_element_type=F32
            )
        high, mid, low = split3(jnp.where(keep, table, 0.0))
        chosen = jnp.where(is_high, high.astype(F32), jnp.where(is_mid, mid.astype(F32), low.astype(F32)))
        lhs_ref[half] = chosen.astype(BF16)

    row = iota((cps, 128), 0)
    ns = jnp.zeros((cps, 128), F32)
    for q in range(cps):
        ns = jnp.where(row == q, scale_s[q] * (-LOG2E), ns)
    ns_ref[...] = ns
    acc_ref[...] = jnp.zeros_like(acc_ref)

    block_gain = decay**dates
    block_square = 0.5 * dt * sum(decay ** (2 * (u + 1)) for u in range(dates))
    row = iota((8, width), 0)
    gain = jnp.where(row == 0, block_gain, 1.0)
    for k in range(CHUNKS):
        all_of(s1_send, s1_recv, k).wait_recv()
        rcv_ref[k, me] = sum_ref[k * n_tm + me]
        state = jnp.zeros((8, width), F32)
        for b in range(n_tm):
            pre_ref[k, b] = state
            if b < n_tm - 1:
                x = rcv_ref[k, b]
                rate = jnp.broadcast_to(state[0:1], (8, width))
                slope = jnp.broadcast_to(x[6:7], (8, width))
                extra = rate * (slope + rate * block_square)
                state = gain * state + jnp.where(row < 6, x, 0.0) + jnp.where(row == 5, extra, 0.0)

        @pl.loop(1, n_tm)
        def _(i):
            send2(k, i).start()

        st_ref[k * n_tm + me] = pre_ref[k, me]

    squares = 0.5 * dt * jnp.exp(2 * log_decay) * (1.0 - jnp.exp(2 * log_decay * (date_col(width) + 1.0))) * (
        1.0 / (1.0 - math.exp(2 * log_decay))
    )
    fill = ones_where(iota((64, width), 0) < 16).astype(BF16)

    def prepare(i, slot):
        state = st_ref[i]
        rate, hazard = state[0:1], state[5:6]
        ab = ab_ref[i]
        haz_ref[slot, 0:dates] = hazard + ab[:dates] + rate * (ab[dates:] + rate * squares)
        for half in range(2):
            spots = []
            for j in range(ccys):
                at = half * 32 + j * 8
                spots.append(jnp.exp(log_ref[i, at : at + 8] + state[1 + j : 2 + j]))
            high, mid, low = split3(jnp.concatenate(spots, axis=0))
            right = jnp.concatenate([high, high, high, mid, mid, low, fill], axis=0)
            net_ref[slot, half] = jnp.dot(lhs_ref[half], right, preferred_element_type=F32)

    def weigh(i, slot):
        scale = jnp.concatenate([ns_ref[...]] * (width // 128), axis=1)
        before = jnp.exp2(scale * st_ref[i, 5:6])
        for t in range(dates):
            now = jnp.exp2(scale * haz_ref[slot, t : t + 1])
            at = (t % 8) * cps
            worth = jnp.maximum(net_ref[slot, t // 8, at : at + cps], 0.0) * (before - now)
            before = now
            total = worth[:, :128]
            for q in range(1, width // 128):
                total = total + worth[:, q * 128 : (q + 1) * 128]
            acc_ref[t * cps : (t + 1) * cps] += total

    for k in range(CHUNKS):
        all_of(s2_send, s2_recv, k).wait_recv()

        @pl.loop(0, n_tm)
        def _(o):
            prepare(k * n_tm + o, 0)
            weigh(k * n_tm + o, 0)

    turned = jnp.sum(jnp.transpose(acc_ref[...]), axis=0, keepdims=True)
    part_ref[...] = turned * (1.0 / (total_paths * dt))
    parts_rcv[my_path] = part_ref[...]

    def send_part(i):
        to = lax.rem(my_path + i, n_path)
        return pltpu.make_async_remote_copy(
            src_ref=part_ref,
            dst_ref=parts_rcv.at[my_path],
            send_sem=t_send.at[0],
            recv_sem=t_recv.at[0],
            device_id={"path": to},
            device_id_type=MESH,
        )

    @pl.loop(1, n_path)
    def _(i):
        send_part(i).start()

    def all_parts(ref, n, at, where):
        return pltpu.make_async_remote_copy(
            src_ref=ref.at[pl.ds(0, n - 1)],
            dst_ref=ref.at[pl.ds(0, n - 1)],
            send_sem=t_send.at[at],
            recv_sem=t_recv.at[at],
            device_id=where,
            device_id_type=MESH,
        )

    lane = iota((1, dates * cps), 1)
    at_date = (lane // cps + me * dates).astype(F32)
    discount = (LOSS_SHARE * dt) * jnp.exp(-RATE_DOM * dt * (at_date + 1.0))
    all_parts(parts_rcv, n_path, 0, {"path": my_path}).wait_recv()
    profile = parts_rcv[0]
    for q in range(1, n_path):
        profile = profile + parts_rcv[q]
    prof_out[...] = profile
    terms = profile * discount
    total = terms[:, :128]
    for q in range(1, dates * cps // 128):
        total = total + terms[:, q * 128 : (q + 1) * 128]
    total = total + pltpu.roll(total, 64, 1)
    total = total + pltpu.roll(total, 32, 1)
    cpart_ref[...] = total
    cparts_rcv[me] = total

    def send_cva(i):
        to = lax.rem(me + i, n_tm)
        return pltpu.make_async_remote_copy(
            src_ref=cpart_ref,
            dst_ref=cparts_rcv.at[me],
            send_sem=t_send.at[1],
            recv_sem=t_recv.at[1],
            device_id={"tm": to},
            device_id_type=MESH,
        )

    @pl.loop(1, n_tm)
    def _(i):
        send_cva(i).start()

    for k in range(CHUNKS):
        all_of(s1_send, s1_recv, k).wait_send()
        all_of(s2_send, s2_recv, k).wait_send()
    all_parts(parts_rcv, n_path, 0, {"path": my_path}).wait_send()
    all_parts(cparts_rcv, n_tm, 1, {"tm": me}).wait_recv()
    cva = cparts_rcv[0]
    for q in range(1, n_tm):
        cva = cva + cparts_rcv[q]
    cva_out[...] = cva
    all_parts(cparts_rcv, n_tm, 1, {"tm": me}).wait_send()


def per_device(n_tm, n_path, shock_rate, shock_fx, fx_vol, fx_corr, hazard_scale, *trades):
    dates, paths = shock_rate.shape
    ccys, cps = fx_vol.shape[0], hazard_scale.shape[0]
    geometry = (n_tm, n_path, paths, dates, cps, ccys, dates * n_tm, paths * n_path)
    width = paths // (CHUNKS * n_tm)
    tiles = CHUNKS * n_tm
    count = trades[0].shape[0]
    vmem = functools.partial(pl.BlockSpec, memory_space=pltpu.VMEM)
    smem = functools.partial(pl.BlockSpec, memory_space=pltpu.SMEM)
    anywhere = functools.partial(pl.BlockSpec, memory_space=pl.ANY)
    sems = pltpu.SemaphoreType.DMA
    profile, cva = pl.pallas_call(
        functools.partial(kernel, geometry),
        out_shape=(
            jax.ShapeDtypeStruct((1, dates * cps), F32),
            jax.ShapeDtypeStruct((1, 128), F32),
        ),
        in_specs=[anywhere(), anywhere(), smem(), smem(), smem()] + [vmem()] * 5,
        out_specs=(vmem(), vmem()),
        scratch_shapes=[
            pltpu.VMEM((dates, paths), F32),
            pltpu.VMEM((ccys, dates, paths), F32),
            pltpu.VMEM((tiles, 64, width), F32),
            pltpu.VMEM((tiles, 32, width), F32),
            pltpu.VMEM((tiles, 8, width), F32),
            pltpu.VMEM((CHUNKS, n_tm, 8, width), F32),
            pltpu.VMEM((CHUNKS, n_tm, 8, width), F32),
            pltpu.VMEM((tiles, 8, width), F32),
            pltpu.VMEM((96, 256), BF16),
            pltpu.VMEM((48, 128), BF16),
            pltpu.VMEM((2, 256, 256), BF16),
            pltpu.VMEM((dates, count), F32),
            pltpu.VMEM((dates, count), F32),
            pltpu.VMEM((cps, 128), F32),
            pltpu.VMEM((2, 2, 256, width), F32),
            pltpu.VMEM((2, dates, width), F32),
            pltpu.VMEM((dates * cps, 128), F32),
            pltpu.VMEM((1, dates * cps), F32),
            pltpu.VMEM((n_path, 1, dates * cps), F32),
            pltpu.VMEM((1, 128), F32),
            pltpu.VMEM((n_tm, 1, 128), F32),
            sems((2, CHUNKS)),
            sems((CHUNKS,)),
            sems((CHUNKS,)),
            sems((CHUNKS,)),
            sems((CHUNKS,)),
            sems((2,)),
            sems((2,)),
        ],
        compiler_params=pltpu.CompilerParams(collective_id=0, has_side_effects=True),
    )(shock_rate, shock_fx, fx_vol, fx_corr, hazard_scale, *(a.reshape(1, count) for a in trades))
    return profile.reshape(dates, cps), cva[0, :cps]


def solution(mesh):
    placed = (P("tm", "path"), P(None, "tm", "path"), P(), P(), P(), P(), P(), P(), P(), P())
    return jax.shard_map(
        functools.partial(per_device, mesh.shape["tm"], mesh.shape["path"]),
        mesh=mesh,
        in_specs=placed,
        out_specs=(P("tm", None), P()),
        check_vma=False,
    )
```

```python
import functools
import math

import jax
import jax.numpy as jnp
from jax import lax
from jax.experimental import pallas as pl
from jax.experimental.pallas import tpu as pltpu
from jax.sharding import PartitionSpec as P

HORIZON = 5.0
RATE_DOM = 0.03
RATE_FOR = 0.01
LOSS_SHARE = 0.6
RATE_SHIFT = 1.5
LOG2E = 1.4426950408889634

CHUNKS = 4
GROUP = 2048
MESH = pl.DeviceIdType.MESH
F32 = jnp.float32
BF16 = jnp.bfloat16


def split3(x):
    high = x.astype(BF16)
    rest = x - high.astype(F32)
    mid = rest.astype(BF16)
    low = (rest - mid.astype(F32)).astype(BF16)
    return high, mid, low


def iota(shape, dim):
    return lax.broadcasted_iota(jnp.int32, shape, dim)


def ring_far(i, n):
    return min(i, n - i)


def tm_order(n):
    return sorted(range(1, n), key=lambda i: -(ring_far(i // 4, n // 4) + ring_far(i % 4, 4)))


def path_order(n):
    return sorted(range(1, n), key=lambda i: -ring_far(i, n))


def ones_where(mask):
    return jnp.where(mask, 1.0, 0.0)


def kernel(
    geometry,
    rate_hbm, fx_hbm, vol_hbm, corr_hbm, scale_hbm, cp_hbm, ccy_hbm, mat_hbm, notl_hbm, strike_hbm,
    prof_out, cva_out,
    xr, xf, log_ref, ab_ref, sum_ref, rcv_ref, pre_ref, st_ref,
    m1_ref, m2_ref, lhs_ref, wf_ref, wd_ref, ns_ref, net0_ref, net1_ref, haz0_ref, haz1_ref, acc_ref,
    part_ref, parts_rcv, cpart_ref, cparts_rcv,
    vol_s, corr_s, scale_s, cp_ref, ccy_ref, mat_ref, notl_ref, strike_ref,
    in_sem, small_sem, s1_send, s1_recv, s2_send, s2_recv, t_send, t_recv,
):
    n_tm, n_path, paths, dates, cps, ccys, total_dates, total_paths = geometry
    dt = HORIZON / total_dates
    decay = math.exp(-2.0 / total_dates)
    noise = math.sqrt(1.0 - decay * decay)
    width = paths // (CHUNKS * n_tm)
    tiles = CHUNKS * n_tm
    chunk_paths = n_tm * width
    group = min(GROUP, chunk_paths)
    me = lax.axis_index("tm")
    my_path = lax.axis_index("path")

    def load_copies(k):
        lanes = pl.ds(k * chunk_paths, chunk_paths)
        return (
            pltpu.make_async_copy(rate_hbm.at[:, lanes], xr.at[:, lanes], in_sem.at[0, k]),
            pltpu.make_async_copy(fx_hbm.at[:, :, lanes], xf.at[:, :, lanes], in_sem.at[1, k]),
        )

    small = [
        pltpu.make_async_copy(source, target, small_sem.at[q])
        for q, (source, target) in enumerate(
            zip(
                (vol_hbm, corr_hbm, scale_hbm, cp_hbm, ccy_hbm, mat_hbm, notl_hbm, strike_hbm),
                (vol_s, corr_s, scale_s, cp_ref, ccy_ref, mat_ref, notl_ref, strike_ref),
            )
        )
    ]
    for copy in load_copies(0):
        copy.start()
    for copy in small:
        copy.start()
    for k in range(1, CHUNKS):
        for copy in load_copies(k):
            copy.start()

    barrier = pltpu.get_barrier_semaphore()

    for i in tm_order(n_tm):
        pl.semaphore_signal(barrier, inc=1, device_id={"tm": lax.rem(me + i, n_tm)}, device_id_type=MESH)
    for i in path_order(n_path):
        pl.semaphore_signal(
            barrier, inc=1, device_id={"path": lax.rem(my_path + i, n_path)}, device_id_type=MESH
        )

    r, c = iota((96, 256), 0), iota((96, 256), 1)
    s = c - jnp.where(c >= 80, 80, 0) - jnp.where(c >= 160, 80, 0)
    in_ccy, in_date = (s >> 4) - 1, s & 15
    last = jnp.full_like(r, 15)
    out_ccy = jnp.where(r < 64, (r & 31) >> 3, jnp.where((r < 80) | (r == 80), -1, jnp.where(r < 85, r - 81, 9)))
    out_date = jnp.where(r < 64, ((r >> 5) << 3) + (r & 7), jnp.where(r < 80, r - 64, last))
    m1_ref[...] = ones_where((c < 240) & (in_ccy == out_ccy) & (in_date <= out_date)).astype(BF16)
    r, c = iota((48, 128), 0), iota((48, 128), 1)
    s = c & 31
    in_kind, in_date = s >> 4, s & 15
    out_kind = jnp.where(r < 32, r >> 4, jnp.where(r == 37, 0, jnp.where(r == 38, 1, 9)))
    out_date = jnp.where(r < 32, r & 15, jnp.full_like(r, 15))
    m2_ref[...] = ones_where((c < 96) & (in_kind == out_kind) & (in_date <= out_date)).astype(BF16)

    small[0].wait()
    small[1].wait()

    def vec(ref, j):
        return jnp.full((1, 128), ref[j], F32)

    def wide(v, n):
        return jnp.broadcast_to(v[:, :1], (v.shape[0], n))

    c_rate, c_own, c_drift = [], [], []
    for j in range(ccys):
        vol, corr = vec(vol_s, j), vec(corr_s, j)
        c_rate.append(wide(vol * (LOG2E * math.sqrt(dt)) * corr, group))
        c_own.append(wide(vol * (LOG2E * math.sqrt(dt)) * jnp.sqrt(1.0 - corr * corr), group))
        c_drift.append(wide((0.5 * LOG2E * dt) * vol * vol, group))

    def date_col(n):
        return iota((dates, n), 0).astype(F32)

    log_decay = -2.0 / total_dates

    def walk(first, k, u):
        lanes = pl.ds(pl.multiple_of(first, group), group)
        rate = xr[:, lanes]
        rows = [rate * (noise * jnp.exp(-log_decay * date_col(group)))]
        for j in range(ccys):
            rows.append((c_rate[j] * rate + c_own[j] * xf[j, :, lanes]) - c_drift[j])
        high, mid, low = split3(jnp.concatenate(rows, axis=0))
        right = jnp.concatenate([high, mid, low, jnp.zeros((16, group), BF16)], axis=0)
        out = jnp.dot(m1_ref[...], right, preferred_element_type=F32)
        power = jnp.exp(log_decay * date_col(group))
        shifted = out[64:80] * power + RATE_SHIFT
        cost = dt * (0.1 + 0.5 * shifted * shifted)
        slope = (dt * decay) * power * shifted
        high, mid, low = split3(jnp.concatenate([cost, slope], axis=0))
        right = jnp.concatenate([high, mid, low, jnp.zeros((32, group), BF16)], axis=0)
        out2 = jnp.dot(m2_ref[...], right, preferred_element_type=F32)
        row = iota((8, group), 0)
        ends = jnp.where(row == 0, decay ** (dates - 1), 1.0) * out[80:88] + out2[32:40]
        tile0 = first // width
        for q in range(group // width):
            part = slice(q * width, (q + 1) * width)
            log_ref[tile0 + q] = out[:64, part]
            ab_ref[tile0 + q] = out2[:32, part]
            sum_ref[tile0 + q] = ends[:, part]

    def send1(k, i):
        owner = lax.rem(me + i, n_tm)
        return pltpu.make_async_remote_copy(
            src_ref=sum_ref.at[k * n_tm + owner, pl.ds(0, 7)],
            dst_ref=rcv_ref.at[k, me, pl.ds(0, 7)],
            send_sem=s1_send.at[k],
            recv_sem=s1_recv.at[k],
            device_id={"tm": owner},
            device_id_type=MESH,
        )

    def send2(k, i):
        block = lax.rem(me + i, n_tm)
        return pltpu.make_async_remote_copy(
            src_ref=pre_ref.at[k, block, pl.ds(0, 6)],
            dst_ref=st_ref.at[k * n_tm + me, pl.ds(0, 6)],
            send_sem=s2_send.at[k],
            recv_sem=s2_recv.at[k],
            device_id={"tm": block},
            device_id_type=MESH,
        )

    def all_of(send, recv, k, rows):
        return pltpu.make_async_remote_copy(
            src_ref=rcv_ref.at[k, pl.ds(0, n_tm - 1), pl.ds(0, rows)],
            dst_ref=rcv_ref.at[k, pl.ds(0, n_tm - 1), pl.ds(0, rows)],
            send_sem=send.at[k],
            recv_sem=recv.at[k],
            device_id={"tm": me},
            device_id_type=MESH,
        )

    for k in range(CHUNKS):
        with jax.named_scope(f"inwait{k}"):
            for copy in load_copies(k):
                copy.wait()
        with jax.named_scope(f"walk{k}"):
            for u in range(chunk_paths // group):
                walk(k * chunk_paths + u * group, k, u)
        if k == 0:
            with jax.named_scope("barrier"):
                pl.semaphore_wait(barrier, n_tm - 1 + n_path - 1)

        for i in tm_order(n_tm):
            send1(k, i).start()

    for copy in small[2:]:
        copy.wait()

    cp, ccy, mat = cp_ref[...], ccy_ref[...], mat_ref[...]
    trades = cp.shape[1]
    date = iota((dates, trades), 0) + me * dates
    alive = date < mat
    left = (mat - date).astype(F32) * dt
    notl = notl_ref[...]
    wf_ref[...] = jnp.where(alive, notl * jnp.exp(-RATE_FOR * left), 0.0)
    wd_ref[...] = jnp.where(alive, -(notl * strike_ref[...]) * jnp.exp(-RATE_DOM * left), 0.0)
    member = cp == iota((cps, trades), 0)
    col = iota((256, trades), 0)
    pick = jnp.concatenate(
        [
            ones_where((col < 192) & (ccy == ((col & 31) >> 3))).astype(BF16),
            ones_where((col >= 192) & (col < 195)).astype(BF16),
        ],
        axis=1,
    )
    r, c = iota((256, 256), 0), iota((256, 256), 1)
    keep = (c >= 192) | ((r >> 5) == (c & 7))
    part = c >> 5
    is_high = (part == 0) | (part == 3) | (part == 5) | (c == 192)
    is_mid = (part == 1) | (part == 4) | (c == 193)
    for half in range(2):
        blocks = []
        for t in range(half * 8, half * 8 + 8):
            blocks.append(
                jnp.concatenate(
                    [
                        jnp.where(member, wf_ref[t : t + 1], 0.0),
                        jnp.where(member, wd_ref[t : t + 1], 0.0),
                    ],
                    axis=1,
                )
            )
        table = jnp.zeros((256, 256), F32)
        for piece in split3(jnp.concatenate(blocks, axis=0)):
            table = table + lax.dot_general(
                piece, pick, (((1,), (1,)), ((), ())), preferred_element_type=F32
            )
        high, mid, low = split3(jnp.where(keep, table, 0.0))
        chosen = jnp.where(is_high, high.astype(F32), jnp.where(is_mid, mid.astype(F32), low.astype(F32)))
        lhs_ref[half] = chosen.astype(BF16)

    row = iota((cps, 128), 0)
    ns = jnp.zeros((cps, 128), F32)
    for q in range(cps):
        ns = jnp.where(row == q, scale_s[q] * (-LOG2E), ns)
    ns_ref[...] = ns
    acc_ref[...] = jnp.zeros_like(acc_ref)

    block_gain = decay**dates
    block_square = 0.5 * dt * sum(decay ** (2 * (u + 1)) for u in range(dates))
    row = iota((8, width), 0)
    gain = jnp.where(row == 0, block_gain, 1.0)
    for k in range(CHUNKS):
        with jax.named_scope(f"wait1_{k}"):
            all_of(s1_send, s1_recv, k, 7).wait_recv()
        rcv_ref[k, me] = sum_ref[k * n_tm + me]
        state = jnp.zeros((8, width), F32)
        for b in range(n_tm):
            pre_ref[k, b] = state
            if b < n_tm - 1:
                x = rcv_ref[k, b]
                rate = jnp.broadcast_to(state[0:1], (8, width))
                slope = jnp.broadcast_to(x[6:7], (8, width))
                extra = rate * (slope + rate * block_square)
                state = gain * state + jnp.where(row < 6, x, 0.0) + jnp.where(row == 5, extra, 0.0)

        for i in tm_order(n_tm):
            send2(k, i).start()

        st_ref[k * n_tm + me] = pre_ref[k, me]

    squares = 0.5 * dt * jnp.exp(2 * log_decay) * (1.0 - jnp.exp(2 * log_decay * (date_col(width) + 1.0))) * (
        1.0 / (1.0 - math.exp(2 * log_decay))
    )
    fill = ones_where(iota((64, width), 0) < 16).astype(BF16)

    nets, hazs = (net0_ref, net1_ref), (haz0_ref, haz1_ref)

    def prepare(i, slot):
        state = st_ref[i]
        rate, hazard = state[0:1], state[5:6]
        ab = ab_ref[i]
        hazs[slot][...] = hazard + ab[:dates] + rate * (ab[dates:] + rate * squares)
        for half in range(2):
            spots = []
            for j in range(ccys):
                at = half * 32 + j * 8
                spots.append(jnp.exp2(log_ref[i, at : at + 8] + state[1 + j : 2 + j]))
            high, mid, low = split3(jnp.concatenate(spots, axis=0))
            right = jnp.concatenate([high, high, high, mid, mid, low, fill], axis=0)
            nets[slot][half] = jnp.dot(lhs_ref[half], right, preferred_element_type=F32)

    def weigh(i, slot):
        scale = jnp.concatenate([ns_ref[...]] * (width // 128), axis=1)
        before = jnp.exp2(scale * st_ref[i, 5:6])
        for t in range(dates):
            now = jnp.exp2(scale * hazs[slot][t : t + 1])
            at = (t % 8) * cps
            worth = jnp.maximum(nets[slot][t // 8, at : at + cps], 0.0) * (before - now)
            before = now
            total = worth[:, :128]
            for q in range(1, width // 128):
                total = total + worth[:, q * 128 : (q + 1) * 128]
            acc_ref[t * cps : (t + 1) * cps] += total

    for k in range(CHUNKS):
        with jax.named_scope(f"wait2_{k}"):
            all_of(s2_send, s2_recv, k, 6).wait_recv()

        with jax.named_scope(f"weigh{k}"):

            first = k * n_tm
            prepare(first, 0)

            @pl.loop(0, n_tm // 2)
            def _(o):
                i = first + 2 * o
                prepare(i + 1, 1)
                weigh(i, 0)
                prepare(jnp.minimum(i + 2, first + n_tm - 1), 0)
                weigh(i + 1, 1)

    turned = jnp.sum(jnp.transpose(acc_ref[...]), axis=0, keepdims=True)
    part_ref[...] = turned * (1.0 / (total_paths * dt))
    parts_rcv[my_path] = part_ref[...]

    def send_part(i):
        to = lax.rem(my_path + i, n_path)
        return pltpu.make_async_remote_copy(
            src_ref=part_ref,
            dst_ref=parts_rcv.at[my_path],
            send_sem=t_send.at[0],
            recv_sem=t_recv.at[0],
            device_id={"path": to},
            device_id_type=MESH,
        )

    for i in path_order(n_path):
        send_part(i).start()

    def all_parts(ref, n, at, where):
        return pltpu.make_async_remote_copy(
            src_ref=ref.at[pl.ds(0, n - 1)],
            dst_ref=ref.at[pl.ds(0, n - 1)],
            send_sem=t_send.at[at],
            recv_sem=t_recv.at[at],
            device_id=where,
            device_id_type=MESH,
        )

    lane = iota((1, dates * cps), 1)
    at_date = (lane // cps + me * dates).astype(F32)
    discount = (LOSS_SHARE * dt) * jnp.exp(-RATE_DOM * dt * (at_date + 1.0))
    with jax.named_scope("wait_t1"):
        all_parts(parts_rcv, n_path, 0, {"path": my_path}).wait_recv()
    profile = parts_rcv[0]
    for q in range(1, n_path):
        profile = profile + parts_rcv[q]
    for t in range(dates):
        prof_out[t : t + 1] = profile[:, t * cps : (t + 1) * cps]
    terms = profile * discount
    total = terms[:, :128]
    for q in range(1, dates * cps // 128):
        total = total + terms[:, q * 128 : (q + 1) * 128]
    total = total + pltpu.roll(total, 64, 1)
    total = total + pltpu.roll(total, 32, 1)
    cpart_ref[...] = total
    cparts_rcv[me] = total

    def send_cva(i):
        to = lax.rem(me + i, n_tm)
        return pltpu.make_async_remote_copy(
            src_ref=cpart_ref,
            dst_ref=cparts_rcv.at[me],
            send_sem=t_send.at[1],
            recv_sem=t_recv.at[1],
            device_id={"tm": to},
            device_id_type=MESH,
        )

    for i in tm_order(n_tm):
        send_cva(i).start()

    for k in range(CHUNKS):
        all_of(s1_send, s1_recv, k, 7).wait_send()
        all_of(s2_send, s2_recv, k, 6).wait_send()
    all_parts(parts_rcv, n_path, 0, {"path": my_path}).wait_send()
    with jax.named_scope("wait_t2"):
        all_parts(cparts_rcv, n_tm, 1, {"tm": me}).wait_recv()
    cva = cparts_rcv[0]
    for q in range(1, n_tm):
        cva = cva + cparts_rcv[q]
    cva_out[...] = cva[:, :cps]
    all_parts(cparts_rcv, n_tm, 1, {"tm": me}).wait_send()


def per_device(n_tm, n_path, shock_rate, shock_fx, fx_vol, fx_corr, hazard_scale, *trades):
    dates, paths = shock_rate.shape
    ccys, cps = fx_vol.shape[0], hazard_scale.shape[0]
    geometry = (n_tm, n_path, paths, dates, cps, ccys, dates * n_tm, paths * n_path)
    width = paths // (CHUNKS * n_tm)
    tiles = CHUNKS * n_tm
    count = trades[0].shape[0]
    vmem = functools.partial(pl.BlockSpec, memory_space=pltpu.VMEM)
    anywhere = functools.partial(pl.BlockSpec, memory_space=pl.ANY)
    sems = pltpu.SemaphoreType.DMA
    profile, cva = pl.pallas_call(
        functools.partial(kernel, geometry),
        out_shape=(
            jax.ShapeDtypeStruct((dates, cps), F32),
            jax.ShapeDtypeStruct((1, cps), F32),
        ),
        in_specs=[anywhere()] * 10,
        out_specs=(vmem(), vmem()),
        scratch_shapes=[
            pltpu.VMEM((dates, paths), F32),
            pltpu.VMEM((ccys, dates, paths), F32),
            pltpu.VMEM((tiles, 64, width), F32),
            pltpu.VMEM((tiles, 32, width), F32),
            pltpu.VMEM((tiles, 8, width), F32),
            pltpu.VMEM((CHUNKS, n_tm, 8, width), F32),
            pltpu.VMEM((CHUNKS, n_tm, 8, width), F32),
            pltpu.VMEM((tiles, 8, width), F32),
            pltpu.VMEM((96, 256), BF16),
            pltpu.VMEM((48, 128), BF16),
            pltpu.VMEM((2, 256, 256), BF16),
            pltpu.VMEM((dates, count), F32),
            pltpu.VMEM((dates, count), F32),
            pltpu.VMEM((cps, 128), F32),
            pltpu.VMEM((2, 256, width), F32),
            pltpu.VMEM((2, 256, width), F32),
            pltpu.VMEM((dates, width), F32),
            pltpu.VMEM((dates, width), F32),
            pltpu.VMEM((dates * cps, 128), F32),
            pltpu.VMEM((1, dates * cps), F32),
            pltpu.VMEM((n_path, 1, dates * cps), F32),
            pltpu.VMEM((1, 128), F32),
            pltpu.VMEM((n_tm, 1, 128), F32),
            pltpu.SMEM((ccys,), F32),
            pltpu.SMEM((ccys,), F32),
            pltpu.SMEM((cps,), F32),
            pltpu.VMEM((1, count), jnp.int32),
            pltpu.VMEM((1, count), jnp.int32),
            pltpu.VMEM((1, count), jnp.int32),
            pltpu.VMEM((1, count), F32),
            pltpu.VMEM((1, count), F32),
            sems((2, CHUNKS)),
            sems((8,)),
            sems((CHUNKS,)),
            sems((CHUNKS,)),
            sems((CHUNKS,)),
            sems((CHUNKS,)),
            sems((2,)),
            sems((2,)),
        ],
        compiler_params=pltpu.CompilerParams(collective_id=0, has_side_effects=True),
    )(shock_rate, shock_fx, fx_vol, fx_corr, hazard_scale, *(a.reshape(1, count) for a in trades))
    return profile, cva.reshape(cps)


def solution(mesh):
    placed = (P("tm", "path"), P(None, "tm", "path"), P(), P(), P(), P(), P(), P(), P(), P())
    return jax.shard_map(
        functools.partial(per_device, mesh.shape["tm"], mesh.shape["path"]),
        mesh=mesh,
        in_specs=placed,
        out_specs=(P("tm", None), P()),
        check_vma=False,
    )
```

```python
import functools
import math

import jax
import jax.numpy as jnp
from jax import lax
from jax.experimental import pallas as pl
from jax.experimental.pallas import tpu as pltpu
from jax.sharding import PartitionSpec as P

HORIZON = 5.0
RATE_DOM = 0.03
RATE_FOR = 0.01
LOSS_SHARE = 0.6
RATE_SHIFT = 1.5
LOG2E = 1.4426950408889634

CHUNKS = 8
TILE = 256
AHEAD = 4
MESH = pl.DeviceIdType.MESH
F32 = jnp.float32
BF16 = jnp.bfloat16


def split3(x):
    high = x.astype(BF16)
    rest = x - high.astype(F32)
    mid = rest.astype(BF16)
    low = (rest - mid.astype(F32)).astype(BF16)
    return high, mid, low


def iota(shape, dim):
    return lax.broadcasted_iota(jnp.int32, shape, dim)


def ring_far(i, n):
    return min(i, n - i)


def tm_order(n):
    return sorted(range(1, n), key=lambda i: -(ring_far(i // 4, n // 4) + ring_far(i % 4, 4)))


def path_order(n):
    return sorted(range(1, n), key=lambda i: -ring_far(i, n))


def ones_where(mask):
    return jnp.where(mask, 1.0, 0.0)


def kernel(
    geometry,
    rate_hbm, fx_hbm, vol_hbm, corr_hbm, scale_hbm, cp_hbm, ccy_hbm, mat_hbm, notl_hbm, strike_hbm,
    prof_out, cva_out,
    xr, xf, log_ref, ab_ref, sum_ref, rcv_ref, pre_ref, st_ref,
    m1_ref, m2_ref, lhs_ref, wf_ref, wd_ref, ns_ref, net0_ref, net1_ref, net2_ref, net3_ref, haz0_ref, haz1_ref, haz2_ref, haz3_ref, acc_ref,
    part_ref, parts_rcv, cpart_ref, cparts_rcv,
    vol_s, corr_s, scale_s, cp_ref, ccy_ref, mat_ref, notl_ref, strike_ref,
    in_sem, small_sem, s1_send, s1_recv, s2_send, s2_recv, t_send, t_recv,
):
    n_tm, n_path, paths, dates, cps, ccys, total_dates, total_paths = geometry
    dt = HORIZON / total_dates
    decay = math.exp(-2.0 / total_dates)
    noise = math.sqrt(1.0 - decay * decay)
    piece = paths // (CHUNKS * n_tm)
    width = TILE
    tiles = paths // width
    per_tile = width // piece
    group = chunk_paths = n_tm * piece
    me = lax.axis_index("tm")
    my_path = lax.axis_index("path")

    def load_copies(k):
        lanes = pl.ds(k * chunk_paths, chunk_paths)
        return (
            pltpu.make_async_copy(rate_hbm.at[:, lanes], xr.at[:, lanes], in_sem.at[0, k]),
            pltpu.make_async_copy(fx_hbm.at[:, :, lanes], xf.at[:, :, lanes], in_sem.at[1, k]),
        )

    small = [
        pltpu.make_async_copy(source, target, small_sem.at[q])
        for q, (source, target) in enumerate(
            zip(
                (vol_hbm, corr_hbm, scale_hbm, cp_hbm, ccy_hbm, mat_hbm, notl_hbm, strike_hbm),
                (vol_s, corr_s, scale_s, cp_ref, ccy_ref, mat_ref, notl_ref, strike_ref),
            )
        )
    ]
    for copy in load_copies(0):
        copy.start()
    for copy in small:
        copy.start()
    for k in range(1, CHUNKS):
        for copy in load_copies(k):
            copy.start()

    barrier = pltpu.get_barrier_semaphore()

    for i in tm_order(n_tm):
        pl.semaphore_signal(barrier, inc=1, device_id={"tm": lax.rem(me + i, n_tm)}, device_id_type=MESH)
    for i in path_order(n_path):
        pl.semaphore_signal(
            barrier, inc=1, device_id={"path": lax.rem(my_path + i, n_path)}, device_id_type=MESH
        )

    r, c = iota((96, 256), 0), iota((96, 256), 1)
    s = c - jnp.where(c >= 80, 80, 0) - jnp.where(c >= 160, 80, 0)
    in_ccy, in_date = (s >> 4) - 1, s & 15
    last = jnp.full_like(r, 15)
    out_ccy = jnp.where(r < 64, (r & 31) >> 3, jnp.where((r < 80) | (r == 80), -1, jnp.where(r < 85, r - 81, 9)))
    out_date = jnp.where(r < 64, ((r >> 5) << 3) + (r & 7), jnp.where(r < 80, r - 64, last))
    m1_ref[...] = ones_where((c < 240) & (in_ccy == out_ccy) & (in_date <= out_date)).astype(BF16)
    r, c = iota((48, 128), 0), iota((48, 128), 1)
    s = c & 31
    in_kind, in_date = s >> 4, s & 15
    out_kind = jnp.where(r < 32, r >> 4, jnp.where(r == 37, 0, jnp.where(r == 38, 1, 9)))
    out_date = jnp.where(r < 32, r & 15, jnp.full_like(r, 15))
    m2_ref[...] = ones_where((c < 96) & (in_kind == out_kind) & (in_date <= out_date)).astype(BF16)

    small[0].wait()
    small[1].wait()

    def vec(ref, j):
        return jnp.full((1, 128), ref[j], F32)

    def wide(v, n):
        return jnp.broadcast_to(v[:, :1], (v.shape[0], n))

    c_rate, c_own, c_drift = [], [], []
    for j in range(ccys):
        vol, corr = vec(vol_s, j), vec(corr_s, j)
        c_rate.append(wide(vol * (LOG2E * math.sqrt(dt)) * corr, group))
        c_own.append(wide(vol * (LOG2E * math.sqrt(dt)) * jnp.sqrt(1.0 - corr * corr), group))
        c_drift.append(wide((0.5 * LOG2E * dt) * vol * vol, group))

    def date_col(n):
        return iota((dates, n), 0).astype(F32)

    log_decay = -2.0 / total_dates

    def walk(first):
        lanes = pl.ds(pl.multiple_of(first, group), group)
        rate = xr[:, lanes]
        rows = [rate * (noise * jnp.exp(-log_decay * date_col(group)))]
        for j in range(ccys):
            rows.append((c_rate[j] * rate + c_own[j] * xf[j, :, lanes]) - c_drift[j])
        high, mid, low = split3(jnp.concatenate(rows, axis=0))
        right = jnp.concatenate([high, mid, low, jnp.zeros((16, group), BF16)], axis=0)
        out = jnp.dot(m1_ref[...], right, preferred_element_type=F32)
        power = jnp.exp(log_decay * date_col(group))
        shifted = out[64:80] * power + RATE_SHIFT
        cost = dt * (0.1 + 0.5 * shifted * shifted)
        slope = (dt * decay) * power * shifted
        high, mid, low = split3(jnp.concatenate([cost, slope], axis=0))
        right = jnp.concatenate([high, mid, low, jnp.zeros((32, group), BF16)], axis=0)
        out2 = jnp.dot(m2_ref[...], right, preferred_element_type=F32)
        row = iota((8, group), 0)
        ends = jnp.where(row == 0, decay ** (dates - 1), 1.0) * out[80:88] + out2[32:40]
        for q in range(group // width):
            part = slice(q * width, (q + 1) * width)
            log_ref[first // width + q] = out[:64, part]
            ab_ref[first // width + q] = out2[:32, part]
        for q in range(n_tm):
            sum_ref[first // piece + q] = ends[:, q * piece : (q + 1) * piece]

    def send1(k, i):
        owner = lax.rem(me + i, n_tm)
        return pltpu.make_async_remote_copy(
            src_ref=sum_ref.at[k * n_tm + owner, pl.ds(0, 7)],
            dst_ref=rcv_ref.at[k, me, pl.ds(0, 7)],
            send_sem=s1_send.at[k],
            recv_sem=s1_recv.at[k],
            device_id={"tm": owner},
            device_id_type=MESH,
        )

    def send2(k, i):
        block = lax.rem(me + i, n_tm)
        return pltpu.make_async_remote_copy(
            src_ref=pre_ref.at[k, block, pl.ds(0, 6)],
            dst_ref=st_ref.at[k * n_tm + me, pl.ds(0, 6)],
            send_sem=s2_send.at[k],
            recv_sem=s2_recv.at[k],
            device_id={"tm": block},
            device_id_type=MESH,
        )

    def all_of(send, recv, k, rows):
        return pltpu.make_async_remote_copy(
            src_ref=rcv_ref.at[k, pl.ds(0, n_tm - 1), pl.ds(0, rows)],
            dst_ref=rcv_ref.at[k, pl.ds(0, n_tm - 1), pl.ds(0, rows)],
            send_sem=send.at[k],
            recv_sem=recv.at[k],
            device_id={"tm": me},
            device_id_type=MESH,
        )

    def walk_and_send(k):
        with jax.named_scope(f"inwait{k}"):
            for copy in load_copies(k):
                copy.wait()
        with jax.named_scope(f"walk{k}"):
            walk(k * chunk_paths)
        if k == 0:
            with jax.named_scope("barrier"):
                pl.semaphore_wait(barrier, n_tm - 1 + n_path - 1)
        for i in tm_order(n_tm):
            send1(k, i).start()

    block_gain = decay**dates
    block_square = 0.5 * dt * sum(decay ** (2 * (u + 1)) for u in range(dates))
    kind = iota((8, piece), 0)
    gain = jnp.where(kind == 0, block_gain, 1.0)

    def own(k):
        with jax.named_scope("wait1"):
            all_of(s1_send, s1_recv, k, 7).wait_recv()
        rcv_ref[k, me] = sum_ref[k * n_tm + me]
        state = jnp.zeros((8, piece), F32)
        for b in range(n_tm):
            pre_ref[k, b] = state
            if b < n_tm - 1:
                x = rcv_ref[k, b]
                rate = jnp.broadcast_to(state[0:1], (8, piece))
                slope = jnp.broadcast_to(x[6:7], (8, piece))
                extra = rate * (slope + rate * block_square)
                state = gain * state + jnp.where(kind < 6, x, 0.0) + jnp.where(kind == 5, extra, 0.0)
        for i in tm_order(n_tm):
            send2(k, i).start()
        st_ref[k * n_tm + me] = pre_ref[k, me]

    for k in range(6):
        walk_and_send(k)
    own(0)
    walk_and_send(6)
    own(1)
    walk_and_send(7)

    for copy in small[2:]:
        copy.wait()

    cp, ccy, mat = cp_ref[...], ccy_ref[...], mat_ref[...]
    trades = cp.shape[1]
    date = iota((dates, trades), 0) + me * dates
    alive = date < mat
    left = (mat - date).astype(F32) * dt
    notl = notl_ref[...]
    wf_ref[...] = jnp.where(alive, notl * jnp.exp(-RATE_FOR * left), 0.0)
    wd_ref[...] = jnp.where(alive, -(notl * strike_ref[...]) * jnp.exp(-RATE_DOM * left), 0.0)
    member = cp == iota((cps, trades), 0)
    col = iota((256, trades), 0)
    pick = jnp.concatenate(
        [
            ones_where((col < 192) & (ccy == ((col & 31) >> 3))).astype(BF16),
            ones_where((col >= 192) & (col < 195)).astype(BF16),
        ],
        axis=1,
    )
    r, c = iota((256, 256), 0), iota((256, 256), 1)
    keep = (c >= 192) | ((r >> 5) == (c & 7))
    part = c >> 5
    is_high = (part == 0) | (part == 3) | (part == 5) | (c == 192)
    is_mid = (part == 1) | (part == 4) | (c == 193)
    for half in range(2):
        blocks = []
        for t in range(half * 8, half * 8 + 8):
            blocks.append(
                jnp.concatenate(
                    [
                        jnp.where(member, wf_ref[t : t + 1], 0.0),
                        jnp.where(member, wd_ref[t : t + 1], 0.0),
                    ],
                    axis=1,
                )
            )
        table = jnp.zeros((256, 256), F32)
        for term in split3(jnp.concatenate(blocks, axis=0)):
            table = table + lax.dot_general(
                term, pick, (((1,), (1,)), ((), ())), preferred_element_type=F32
            )
        high, mid, low = split3(jnp.where(keep, table, 0.0))
        chosen = jnp.where(is_high, high.astype(F32), jnp.where(is_mid, mid.astype(F32), low.astype(F32)))
        lhs_ref[half] = chosen.astype(BF16)

    row = iota((cps, 128), 0)
    ns = jnp.zeros((cps, 128), F32)
    for q in range(cps):
        ns = jnp.where(row == q, scale_s[q] * (-LOG2E), ns)
    ns_ref[...] = ns
    acc_ref[...] = jnp.zeros_like(acc_ref)

    own(2)
    own(3)

    squares = 0.5 * dt * jnp.exp(2 * log_decay) * (1.0 - jnp.exp(2 * log_decay * (date_col(width) + 1.0))) * (
        1.0 / (1.0 - math.exp(2 * log_decay))
    )
    fill = ones_where(iota((64, width), 0) < 16).astype(BF16)

    nets, hazs = (net0_ref, net1_ref, net2_ref, net3_ref), (haz0_ref, haz1_ref, haz2_ref, haz3_ref)

    def prepare(i, slot):
        state = jnp.concatenate([st_ref[i * per_tile + q] for q in range(per_tile)], axis=1)
        rate, hazard = state[0:1], state[5:6]
        ab = ab_ref[i]
        hazs[slot][...] = hazard + ab[:dates] + rate * (ab[dates:] + rate * squares)
        for half in range(2):
            spots = []
            for j in range(ccys):
                at = half * 32 + j * 8
                spots.append(jnp.exp2(log_ref[i, at : at + 8] + state[1 + j : 2 + j]))
            high, mid, low = split3(jnp.concatenate(spots, axis=0))
            right = jnp.concatenate([high, high, high, mid, mid, low, fill], axis=0)
            nets[slot][half] = jnp.dot(lhs_ref[half], right, preferred_element_type=F32)

    def weigh(tiles):
        for g in range(0, cps, 8):
            scale = ns_ref[g : g + 8]
            before = []
            for i, slot in tiles:
                for q in range(width // 128):
                    place = q * 128 // piece
                    start = q * 128 % piece
                    before.append(jnp.exp2(scale * st_ref[i * per_tile + place, 5:6, start : start + 128]))
            for t in range(dates):
                at = (t % 8) * cps + g
                total = None
                n = 0
                for i, slot in tiles:
                    for q in range(width // 128):
                        lanes = slice(q * 128, (q + 1) * 128)
                        now = jnp.exp2(scale * hazs[slot][t : t + 1, lanes])
                        worth = jnp.maximum(nets[slot][t // 8, at : at + 8, lanes], 0.0) * (before[n] - now)
                        before[n] = now
                        n += 1
                        total = worth if total is None else total + worth
                acc_ref[t * cps + g : t * cps + g + 8] += total

    def wait2(k):
        with jax.named_scope("wait2"):
            all_of(s2_send, s2_recv, k, 6).wait_recv()

    per_chunk = tiles // CHUNKS // 4
    wait2(0)
    prepare(0, 0)
    prepare(1, 1)
    with jax.named_scope("weigh"):

        @pl.loop(0, tiles // 4)
        def _(it):
            k = it // per_chunk

            @pl.when((it % per_chunk == 0) & (k + AHEAD < CHUNKS))
            def _():
                own(k + AHEAD)

            @pl.when((it % per_chunk == per_chunk - 1) & (k + 1 < CHUNKS))
            def _():
                wait2(k + 1)

            i = 4 * it
            prepare(i + 2, 2)
            prepare(i + 3, 3)
            weigh([(i, 0), (i + 1, 1)])
            j = jnp.minimum(i + 4, tiles - 2)
            prepare(j, 0)
            prepare(j + 1, 1)
            weigh([(i + 2, 2), (i + 3, 3)])

    turned = jnp.sum(jnp.transpose(acc_ref[...]), axis=0, keepdims=True)
    part_ref[...] = turned * (1.0 / (total_paths * dt))
    parts_rcv[my_path] = part_ref[...]

    def send_part(i):
        to = lax.rem(my_path + i, n_path)
        return pltpu.make_async_remote_copy(
            src_ref=part_ref,
            dst_ref=parts_rcv.at[my_path],
            send_sem=t_send.at[0],
            recv_sem=t_recv.at[0],
            device_id={"path": to},
            device_id_type=MESH,
        )

    for i in path_order(n_path):
        send_part(i).start()

    def all_parts(ref, n, at, where):
        return pltpu.make_async_remote_copy(
            src_ref=ref.at[pl.ds(0, n - 1)],
            dst_ref=ref.at[pl.ds(0, n - 1)],
            send_sem=t_send.at[at],
            recv_sem=t_recv.at[at],
            device_id=where,
            device_id_type=MESH,
        )

    lane = iota((1, dates * cps), 1)
    at_date = (lane // cps + me * dates).astype(F32)
    discount = (LOSS_SHARE * dt) * jnp.exp(-RATE_DOM * dt * (at_date + 1.0))
    with jax.named_scope("wait_t1"):
        all_parts(parts_rcv, n_path, 0, {"path": my_path}).wait_recv()
    profile = parts_rcv[0]
    for q in range(1, n_path):
        profile = profile + parts_rcv[q]
    for t in range(dates):
        prof_out[t : t + 1] = profile[:, t * cps : (t + 1) * cps]
    terms = profile * discount
    total = terms[:, :128]
    for q in range(1, dates * cps // 128):
        total = total + terms[:, q * 128 : (q + 1) * 128]
    total = total + pltpu.roll(total, 64, 1)
    total = total + pltpu.roll(total, 32, 1)
    cpart_ref[...] = total
    cparts_rcv[me] = total

    def send_cva(i):
        to = lax.rem(me + i, n_tm)
        return pltpu.make_async_remote_copy(
            src_ref=cpart_ref,
            dst_ref=cparts_rcv.at[me],
            send_sem=t_send.at[1],
            recv_sem=t_recv.at[1],
            device_id={"tm": to},
            device_id_type=MESH,
        )

    for i in tm_order(n_tm):
        send_cva(i).start()

    for k in range(CHUNKS):
        all_of(s1_send, s1_recv, k, 7).wait_send()
        all_of(s2_send, s2_recv, k, 6).wait_send()
    all_parts(parts_rcv, n_path, 0, {"path": my_path}).wait_send()
    with jax.named_scope("wait_t2"):
        all_parts(cparts_rcv, n_tm, 1, {"tm": me}).wait_recv()
    cva = cparts_rcv[0]
    for q in range(1, n_tm):
        cva = cva + cparts_rcv[q]
    cva_out[...] = cva[:, :cps]
    all_parts(cparts_rcv, n_tm, 1, {"tm": me}).wait_send()


def per_device(n_tm, n_path, shock_rate, shock_fx, fx_vol, fx_corr, hazard_scale, *trades):
    dates, paths = shock_rate.shape
    ccys, cps = fx_vol.shape[0], hazard_scale.shape[0]
    geometry = (n_tm, n_path, paths, dates, cps, ccys, dates * n_tm, paths * n_path)
    width, piece = TILE, paths // (CHUNKS * n_tm)
    tiles = paths // width
    count = trades[0].shape[0]
    vmem = functools.partial(pl.BlockSpec, memory_space=pltpu.VMEM)
    anywhere = functools.partial(pl.BlockSpec, memory_space=pl.ANY)
    sems = pltpu.SemaphoreType.DMA
    profile, cva = pl.pallas_call(
        functools.partial(kernel, geometry),
        out_shape=(
            pltpu.VMEM((dates, cps), F32),
            pltpu.VMEM((1, cps), F32),
        ),
        in_specs=[anywhere()] * 10,
        out_specs=(vmem(), vmem()),
        scratch_shapes=[
            pltpu.VMEM((dates, paths), F32),
            pltpu.VMEM((ccys, dates, paths), F32),
            pltpu.VMEM((tiles, 64, width), F32),
            pltpu.VMEM((tiles, 32, width), F32),
            pltpu.VMEM((CHUNKS * n_tm, 8, piece), F32),
            pltpu.VMEM((CHUNKS, n_tm, 8, piece), F32),
            pltpu.VMEM((CHUNKS, n_tm, 8, piece), F32),
            pltpu.VMEM((CHUNKS * n_tm, 8, piece), F32),
            pltpu.VMEM((96, 256), BF16),
            pltpu.VMEM((48, 128), BF16),
            pltpu.VMEM((2, 256, 256), BF16),
            pltpu.VMEM((dates, count), F32),
            pltpu.VMEM((dates, count), F32),
            pltpu.VMEM((cps, 128), F32),
            pltpu.VMEM((2, 256, width), F32),
            pltpu.VMEM((2, 256, width), F32),
            pltpu.VMEM((2, 256, width), F32),
            pltpu.VMEM((2, 256, width), F32),
            pltpu.VMEM((dates, width), F32),
            pltpu.VMEM((dates, width), F32),
            pltpu.VMEM((dates, width), F32),
            pltpu.VMEM((dates, width), F32),
            pltpu.VMEM((dates * cps, 128), F32),
            pltpu.VMEM((1, dates * cps), F32),
            pltpu.VMEM((n_path, 1, dates * cps), F32),
            pltpu.VMEM((1, 128), F32),
            pltpu.VMEM((n_tm, 1, 128), F32),
            pltpu.SMEM((ccys,), F32),
            pltpu.SMEM((ccys,), F32),
            pltpu.SMEM((cps,), F32),
            pltpu.VMEM((1, count), jnp.int32),
            pltpu.VMEM((1, count), jnp.int32),
            pltpu.VMEM((1, count), jnp.int32),
            pltpu.VMEM((1, count), F32),
            pltpu.VMEM((1, count), F32),
            sems((2, CHUNKS)),
            sems((8,)),
            sems((CHUNKS,)),
            sems((CHUNKS,)),
            sems((CHUNKS,)),
            sems((CHUNKS,)),
            sems((2,)),
            sems((2,)),
        ],
        compiler_params=pltpu.CompilerParams(collective_id=0, has_side_effects=True),
    )(shock_rate, shock_fx, fx_vol, fx_corr, hazard_scale, *(a.reshape(1, count) for a in trades))
    return profile, cva.reshape(cps)


def solution(mesh):
    placed = (P("tm", "path"), P(None, "tm", "path"), P(), P(), P(), P(), P(), P(), P(), P())
    return jax.shard_map(
        functools.partial(per_device, mesh.shape["tm"], mesh.shape["path"]),
        mesh=mesh,
        in_specs=placed,
        out_specs=(P("tm", None), P()),
        check_vma=False,
    )
```

```python
import functools
import math

import jax
import jax.numpy as jnp
from jax import lax
from jax.experimental import pallas as pl
from jax.experimental.pallas import tpu as pltpu
from jax.sharding import PartitionSpec as P

HORIZON = 5.0
RATE_DOM = 0.03
RATE_FOR = 0.01
LOSS_SHARE = 0.6
RATE_SHIFT = 1.5
LOG2E = 1.4426950408889634

SIZES = (1, 1, 2, 2, 2)
TILE = 256
CROWD = 8
MESH = pl.DeviceIdType.MESH
F32 = jnp.float32
BF16 = jnp.bfloat16


def split3(x):
    high = x.astype(BF16)
    rest = x - high.astype(F32)
    mid = rest.astype(BF16)
    low = (rest - mid.astype(F32)).astype(BF16)
    return high, mid, low


def split2(x):
    high = x.astype(BF16)
    return high, (x - high.astype(F32)).astype(BF16)


def iota(shape, dim):
    return lax.broadcasted_iota(jnp.int32, shape, dim)


def ring_far(i, n):
    return min(i, n - i)


def tm_order(n):
    return sorted(range(1, n), key=lambda i: -(ring_far(i // 4, n // 4) + ring_far(i % 4, 4)))


def path_order(n):
    return sorted(range(1, n), key=lambda i: -ring_far(i, n))


def ones_where(mask):
    return jnp.where(mask, 1.0, 0.0)


def kernel(
    geometry,
    rate_hbm, fx_hbm, vol_hbm, corr_hbm, scale_hbm, cp_hbm, ccy_hbm, mat_hbm, notl_hbm, strike_hbm,
    prof_out, cva_out,
    xr, xf, log_ref, ab_ref, sum_ref, rcv_ref, pre_ref, st_ref,
    m1_ref, m2_ref, lhs_ref, wf_ref, wd_ref, ns_ref, net0_ref, net1_ref, net2_ref, net3_ref, haz0_ref, haz1_ref, haz2_ref, haz3_ref, acc_ref,
    part_ref, parts_rcv, cpart_ref, cparts_rcv,
    vol_s, corr_s, scale_s, cp_ref, ccy_ref, mat_ref, notl_ref, strike_ref,
    in_sem, small_sem, s1_send, s1_recv, s2_send, s2_recv, t_send, t_recv,
):
    n_tm, n_path, paths, dates, cps, ccys, total_dates, total_paths = geometry
    dt = HORIZON / total_dates
    decay = math.exp(-2.0 / total_dates)
    noise = math.sqrt(1.0 - decay * decay)
    width = TILE
    tiles = paths // width
    per_tile = width // 128
    chunks = len(SIZES)
    assert paths == 128 * n_tm * sum(SIZES)
    first = [n_tm * sum(SIZES[:k]) for k in range(chunks + 1)]
    me = lax.axis_index("tm")
    my_path = lax.axis_index("path")

    def load_copies(k):
        lanes = pl.ds(first[k] * 128, (first[k + 1] - first[k]) * 128)
        return (
            pltpu.make_async_copy(rate_hbm.at[:, lanes], xr.at[:, lanes], in_sem.at[0, k]),
            pltpu.make_async_copy(fx_hbm.at[:, :, lanes], xf.at[:, :, lanes], in_sem.at[1, k]),
        )

    small = [
        pltpu.make_async_copy(source, target, small_sem.at[q])
        for q, (source, target) in enumerate(
            zip(
                (vol_hbm, corr_hbm, scale_hbm, cp_hbm, ccy_hbm, mat_hbm, notl_hbm, strike_hbm),
                (vol_s, corr_s, scale_s, cp_ref, ccy_ref, mat_ref, notl_ref, strike_ref),
            )
        )
    ]
    for copy in load_copies(0):
        copy.start()
    for copy in small:
        copy.start()
    for k in range(1, chunks):
        for copy in load_copies(k):
            copy.start()

    barrier = pltpu.get_barrier_semaphore()

    for i in tm_order(n_tm):
        pl.semaphore_signal(barrier, inc=1, device_id={"tm": lax.rem(me + i, n_tm)}, device_id_type=MESH)
    for i in path_order(n_path):
        pl.semaphore_signal(
            barrier, inc=1, device_id={"path": lax.rem(my_path + i, n_path)}, device_id_type=MESH
        )

    r, c = iota((96, 160), 0), iota((96, 160), 1)
    s = c - jnp.where(c >= 80, 80, 0)
    in_ccy, in_date = (s >> 4) - 1, s & 15
    last = jnp.full_like(r, 15)
    out_ccy = jnp.where(r < 64, (r & 31) >> 3, jnp.where((r < 80) | (r == 80), -1, jnp.where(r < 85, r - 81, 9)))
    out_date = jnp.where(r < 64, ((r >> 5) << 3) + (r & 7), jnp.where(r < 80, r - 64, last))
    m1_ref[...] = ones_where((in_ccy == out_ccy) & (in_date <= out_date)).astype(BF16)
    r, c = iota((48, 64), 0), iota((48, 64), 1)
    s = c & 31
    in_kind, in_date = s >> 4, s & 15
    out_kind = jnp.where(r < 32, r >> 4, jnp.where(r == 37, 0, jnp.where(r == 38, 1, 9)))
    out_date = jnp.where(r < 32, r & 15, jnp.full_like(r, 15))
    m2_ref[...] = ones_where((in_kind == out_kind) & (in_date <= out_date)).astype(BF16)

    small[0].wait()
    small[1].wait()

    def vec(ref, j):
        return jnp.full((1, 128), ref[j], F32)

    def wide(v, n):
        return jnp.broadcast_to(v[:, :1], (v.shape[0], n))

    c_rate, c_own, c_drift = [], [], []
    for j in range(ccys):
        vol, corr = vec(vol_s, j), vec(corr_s, j)
        c_rate.append(vol * (LOG2E * math.sqrt(dt)) * corr)
        c_own.append(vol * (LOG2E * math.sqrt(dt)) * jnp.sqrt(1.0 - corr * corr))
        c_drift.append((0.5 * LOG2E * dt) * vol * vol)

    def date_col(n):
        return iota((dates, n), 0).astype(F32)

    log_decay = -2.0 / total_dates

    def walk(k):
        group = (first[k + 1] - first[k]) * 128
        lanes = pl.ds(first[k] * 128, group)
        rate = xr[:, lanes]
        rows = [rate * (noise * jnp.exp(-log_decay * date_col(group)))]
        for j in range(ccys):
            rows.append((wide(c_rate[j], group) * rate + wide(c_own[j], group) * xf[j, :, lanes]) - wide(c_drift[j], group))
        right = jnp.concatenate(split2(jnp.concatenate(rows, axis=0)), axis=0)
        out = jnp.dot(m1_ref[...], right, preferred_element_type=F32)
        power = jnp.exp(log_decay * date_col(group))
        shifted = out[64:80] * power + RATE_SHIFT
        cost = dt * (0.1 + 0.5 * shifted * shifted)
        slope = (dt * decay) * power * shifted
        right = jnp.concatenate(split2(jnp.concatenate([cost, slope], axis=0)), axis=0)
        out2 = jnp.dot(m2_ref[...], right, preferred_element_type=F32)
        row = iota((8, group), 0)
        ends = jnp.where(row == 0, decay ** (dates - 1), 1.0) * out[80:88] + out2[32:40]
        for q in range(group // width):
            part = slice(q * width, (q + 1) * width)
            log_ref[first[k] // per_tile + q] = out[:64, part]
            ab_ref[first[k] // per_tile + q] = out2[:32, part]
        for q in range(group // 128):
            sum_ref[first[k] + q] = ends[:, q * 128 : (q + 1) * 128]

    def columns(k, device):
        return pl.ds(first[k] + device * SIZES[k], SIZES[k])

    def send1(k, i):
        owner = lax.rem(me + i, n_tm)
        return pltpu.make_async_remote_copy(
            src_ref=sum_ref.at[columns(k, owner), pl.ds(0, 7)],
            dst_ref=rcv_ref.at[columns(k, me), pl.ds(0, 7)],
            send_sem=s1_send.at[k],
            recv_sem=s1_recv.at[k],
            device_id={"tm": owner},
            device_id_type=MESH,
        )

    def send2(k, i):
        block = lax.rem(me + i, n_tm)
        return pltpu.make_async_remote_copy(
            src_ref=pre_ref.at[columns(k, block), pl.ds(0, 6)],
            dst_ref=st_ref.at[columns(k, me), pl.ds(0, 6)],
            send_sem=s2_send.at[k],
            recv_sem=s2_recv.at[k],
            device_id={"tm": block},
            device_id_type=MESH,
        )

    def all_of(send, recv, k, rows):
        return pltpu.make_async_remote_copy(
            src_ref=rcv_ref.at[pl.ds(0, (n_tm - 1) * SIZES[k]), pl.ds(0, rows)],
            dst_ref=rcv_ref.at[pl.ds(0, (n_tm - 1) * SIZES[k]), pl.ds(0, rows)],
            send_sem=send.at[k],
            recv_sem=recv.at[k],
            device_id={"tm": me},
            device_id_type=MESH,
        )

    def walk_and_send(k):
        with jax.named_scope(f"inwait{k}"):
            for copy in load_copies(k):
                copy.wait()
        with jax.named_scope(f"walk{k}"):
            walk(k)
        if k == 0:
            with jax.named_scope("barrier"):
                pl.semaphore_wait(barrier, n_tm - 1 + n_path - 1)
        for i in tm_order(n_tm):
            send1(k, i).start()

    block_gain = decay**dates
    block_square = 0.5 * dt * sum(decay ** (2 * (u + 1)) for u in range(dates))
    kind = iota((8, 128), 0)

    def own(k):
        with jax.named_scope(f"wait1_{k}"):
            all_of(s1_send, s1_recv, k, 7).wait_recv()
        rcv_ref[columns(k, me)] = sum_ref[columns(k, me)]
        for q in range(SIZES[k]):
            rate = rest = jnp.zeros((8, 128), F32)
            for b in range(n_tm):
                at = first[k] + b * SIZES[k] + q
                pre_ref[at] = jnp.where(kind == 0, rate, rest)
                if b < n_tm - 1:
                    x = rcv_ref[at]
                    slope = jnp.broadcast_to(x[6:7], (8, 128))
                    rest = rest + (x + jnp.where(kind == 5, rate * (slope + rate * block_square), 0.0))
                    rate = block_gain * rate + jnp.broadcast_to(x[0:1], (8, 128))
        for i in tm_order(n_tm):
            send2(k, i).start()
        st_ref[columns(k, me)] = pre_ref[columns(k, me)]

    for k in range(chunks):
        walk_and_send(k)
    own(0)

    for copy in small[2:]:
        copy.wait()

    cp, ccy, mat = cp_ref[...], ccy_ref[...], mat_ref[...]
    trades = cp.shape[1]
    date = iota((dates, trades), 0) + me * dates
    alive = date < mat
    left = (mat - date).astype(F32) * dt
    notl = notl_ref[...]
    wf_ref[...] = jnp.where(alive, notl * jnp.exp(-RATE_FOR * left), 0.0)
    wd_ref[...] = jnp.where(alive, -(notl * strike_ref[...]) * jnp.exp(-RATE_DOM * left), 0.0)
    member = cp == iota((cps, trades), 0)
    col = iota((256, trades), 0)
    pick = jnp.concatenate(
        [
            ones_where((col < 160) & (ccy == ((col & 31) >> 3))).astype(BF16),
            ones_where((col >= 160) & (col < 163)).astype(BF16),
        ],
        axis=1,
    )
    r, c = iota((256, 256), 0), iota((256, 256), 1)
    keep = (c >= 160) | ((r >> 5) == (c & 7))
    part = c >> 5
    is_high = (part == 0) | (part == 3) | (c == 160)
    is_mid = (part == 1) | (part == 4) | (c == 161)
    for half in range(2):
        blocks = []
        for t in range(half * 8, half * 8 + 8):
            blocks.append(
                jnp.concatenate(
                    [
                        jnp.where(member, wf_ref[t : t + 1], 0.0),
                        jnp.where(member, wd_ref[t : t + 1], 0.0),
                    ],
                    axis=1,
                )
            )
        table = jnp.zeros((256, 256), F32)
        for term in split3(jnp.concatenate(blocks, axis=0)):
            table = table + lax.dot_general(
                term, pick, (((1,), (1,)), ((), ())), preferred_element_type=F32
            )
        high, mid, low = split3(jnp.where(keep, table, 0.0))
        chosen = jnp.where(is_high, high.astype(F32), jnp.where(is_mid, mid.astype(F32), low.astype(F32)))
        lhs_ref[half] = chosen.astype(BF16)[:, :176]

    row = iota((cps, 128), 0)
    ns = jnp.zeros((cps, 128), F32)
    for q in range(cps):
        ns = jnp.where(row == q, scale_s[q] * (-LOG2E), ns)
    for t in range(dates):
        ns_ref[t] = ns
    acc_ref[...] = jnp.zeros_like(acc_ref)

    for k in range(1, chunks):
        own(k)

    squares = 0.5 * dt * jnp.exp(2 * log_decay) * (1.0 - jnp.exp(2 * log_decay * (date_col(width) + 1.0))) * (
        1.0 / (1.0 - math.exp(2 * log_decay))
    )
    fill = jnp.ones((16, width), BF16)

    nets, hazs = (net0_ref, net1_ref, net2_ref, net3_ref), (haz0_ref, haz1_ref, haz2_ref, haz3_ref)

    def prepare(i, slot):
        state = jnp.concatenate([st_ref[i * per_tile + q] for q in range(per_tile)], axis=1)
        rate, hazard = state[0:1], state[5:6]
        ab = ab_ref[i]
        hazs[slot][...] = hazard + ab[:dates] + rate * (ab[dates:] + rate * squares)
        for half in range(2):
            spots = []
            for j in range(ccys):
                at = half * 32 + j * 8
                spots.append(jnp.exp2(log_ref[i, at : at + 8] + state[1 + j : 2 + j]))
            high, mid = split2(jnp.concatenate(spots, axis=0))
            right = jnp.concatenate([high, high, high, mid, mid, fill], axis=0)
            nets[slot][half] = jnp.dot(lhs_ref[half], right, preferred_element_type=F32)

    def weigh(tiles):
        for g in range(0, cps, CROWD):
            scale = ns_ref[0, g : g + CROWD]
            before = []
            for i, slot in tiles:
                for q in range(width // 128):
                    before.append(jnp.exp2(scale * st_ref[i * per_tile + q, 5:6]))
            for t in range(dates):
                at = (t % 8) * cps + g
                total = None
                n = 0
                for i, slot in tiles:
                    for q in range(width // 128):
                        lanes = slice(q * 128, (q + 1) * 128)
                        now = jnp.exp2(ns_ref[t, g : g + CROWD] * hazs[slot][t : t + 1, lanes])
                        worth = jnp.maximum(nets[slot][t // 8, at : at + CROWD, lanes], 0.0) * (before[n] - now)
                        before[n] = now
                        n += 1
                        total = worth if total is None else total + worth
                acc_ref[t * cps + g : t * cps + g + CROWD] += total

    def wait2(k):
        with jax.named_scope(f"wait2_{k}"):
            all_of(s2_send, s2_recv, k, 6).wait_recv()

    wait2(0)
    prepare(0, 0)
    prepare(1, 1)
    with jax.named_scope("weigh"):

        @pl.loop(0, tiles // 4)
        def _(it):
            for k in range(1, chunks):

                @pl.when(it == first[k] // per_tile // 4 - 1)
                def _():
                    wait2(k)

            i = 4 * it
            prepare(i + 2, 2)
            prepare(i + 3, 3)
            weigh([(i, 0), (i + 1, 1)])
            j = jnp.minimum(i + 4, tiles - 2)
            prepare(j, 0)
            prepare(j + 1, 1)
            weigh([(i + 2, 2), (i + 3, 3)])

    turned = jnp.sum(jnp.transpose(acc_ref[...]), axis=0, keepdims=True)
    part_ref[...] = turned * (1.0 / (total_paths * dt))
    parts_rcv[my_path] = part_ref[...]

    def send_part(i):
        to = lax.rem(my_path + i, n_path)
        return pltpu.make_async_remote_copy(
            src_ref=part_ref,
            dst_ref=parts_rcv.at[my_path],
            send_sem=t_send.at[0],
            recv_sem=t_recv.at[0],
            device_id={"path": to},
            device_id_type=MESH,
        )

    for i in path_order(n_path):
        send_part(i).start()

    def all_parts(ref, n, at, where):
        return pltpu.make_async_remote_copy(
            src_ref=ref.at[pl.ds(0, n - 1)],
            dst_ref=ref.at[pl.ds(0, n - 1)],
            send_sem=t_send.at[at],
            recv_sem=t_recv.at[at],
            device_id=where,
            device_id_type=MESH,
        )

    lane = iota((1, dates * cps), 1)
    at_date = (lane // cps + me * dates).astype(F32)
    discount = (LOSS_SHARE * dt) * jnp.exp(-RATE_DOM * dt * (at_date + 1.0))
    with jax.named_scope("wait_t1"):
        all_parts(parts_rcv, n_path, 0, {"path": my_path}).wait_recv()
    profile = parts_rcv[0]
    for q in range(1, n_path):
        profile = profile + parts_rcv[q]
    for t in range(dates):
        prof_out[t : t + 1] = profile[:, t * cps : (t + 1) * cps]
    terms = profile * discount
    total = terms[:, :128]
    for q in range(1, dates * cps // 128):
        total = total + terms[:, q * 128 : (q + 1) * 128]
    total = total + pltpu.roll(total, 64, 1)
    total = total + pltpu.roll(total, 32, 1)
    cpart_ref[...] = total
    cparts_rcv[me] = total

    def send_cva(i):
        to = lax.rem(me + i, n_tm)
        return pltpu.make_async_remote_copy(
            src_ref=cpart_ref,
            dst_ref=cparts_rcv.at[me],
            send_sem=t_send.at[1],
            recv_sem=t_recv.at[1],
            device_id={"tm": to},
            device_id_type=MESH,
        )

    for i in tm_order(n_tm):
        send_cva(i).start()

    for k in range(chunks):
        all_of(s1_send, s1_recv, k, 7).wait_send()
        all_of(s2_send, s2_recv, k, 6).wait_send()
    all_parts(parts_rcv, n_path, 0, {"path": my_path}).wait_send()
    with jax.named_scope("wait_t2"):
        all_parts(cparts_rcv, n_tm, 1, {"tm": me}).wait_recv()
    cva = cparts_rcv[0]
    for q in range(1, n_tm):
        cva = cva + cparts_rcv[q]
    cva_out[...] = cva[:, :cps]
    all_parts(cparts_rcv, n_tm, 1, {"tm": me}).wait_send()


def hand_out(profile, cva, profile_out, cva_out, sems):
    copies = [
        pltpu.make_async_copy(profile, profile_out, sems.at[0]),
        pltpu.make_async_copy(cva, cva_out, sems.at[1]),
    ]
    for copy in copies:
        copy.start()
    for copy in copies:
        copy.wait()


def per_device(n_tm, n_path, shock_rate, shock_fx, fx_vol, fx_corr, hazard_scale, *trades):
    dates, paths = shock_rate.shape
    ccys, cps = fx_vol.shape[0], hazard_scale.shape[0]
    geometry = (n_tm, n_path, paths, dates, cps, ccys, dates * n_tm, paths * n_path)
    width = TILE
    tiles, columns, chunks = paths // width, paths // 128, len(SIZES)
    count = trades[0].shape[0]
    vmem = functools.partial(pl.BlockSpec, memory_space=pltpu.VMEM)
    anywhere = functools.partial(pl.BlockSpec, memory_space=pl.ANY)
    sems = pltpu.SemaphoreType.DMA
    profile, cva = pl.pallas_call(
        functools.partial(kernel, geometry),
        out_shape=(
            pltpu.VMEM((dates, cps), F32),
            pltpu.VMEM((1, cps), F32),
        ),
        in_specs=[anywhere()] * 10,
        out_specs=(vmem(), vmem()),
        scratch_shapes=[
            pltpu.VMEM((dates, paths), F32),
            pltpu.VMEM((ccys, dates, paths), F32),
            pltpu.VMEM((tiles, 64, width), F32),
            pltpu.VMEM((tiles, 32, width), F32),
            pltpu.VMEM((columns, 8, 128), F32),
            pltpu.VMEM((columns, 8, 128), F32),
            pltpu.VMEM((columns, 8, 128), F32),
            pltpu.VMEM((columns, 8, 128), F32),
            pltpu.VMEM((96, 160), BF16),
            pltpu.VMEM((48, 64), BF16),
            pltpu.VMEM((2, 256, 176), BF16),
            pltpu.VMEM((dates, count), F32),
            pltpu.VMEM((dates, count), F32),
            pltpu.VMEM((dates, cps, 128), F32),
            pltpu.VMEM((2, 256, width), F32),
            pltpu.VMEM((2, 256, width), F32),
            pltpu.VMEM((2, 256, width), F32),
            pltpu.VMEM((2, 256, width), F32),
            pltpu.VMEM((dates, width), F32),
            pltpu.VMEM((dates, width), F32),
            pltpu.VMEM((dates, width), F32),
            pltpu.VMEM((dates, width), F32),
            pltpu.VMEM((dates * cps, 128), F32),
            pltpu.VMEM((1, dates * cps), F32),
            pltpu.VMEM((n_path, 1, dates * cps), F32),
            pltpu.VMEM((1, 128), F32),
            pltpu.VMEM((n_tm, 1, 128), F32),
            pltpu.SMEM((ccys,), F32),
            pltpu.SMEM((ccys,), F32),
            pltpu.SMEM((cps,), F32),
            pltpu.VMEM((1, count), jnp.int32),
            pltpu.VMEM((1, count), jnp.int32),
            pltpu.VMEM((1, count), jnp.int32),
            pltpu.VMEM((1, count), F32),
            pltpu.VMEM((1, count), F32),
            sems((2, chunks)),
            sems((8,)),
            sems((chunks,)),
            sems((chunks,)),
            sems((chunks,)),
            sems((chunks,)),
            sems((2,)),
            sems((2,)),
        ],
        compiler_params=pltpu.CompilerParams(collective_id=0, has_side_effects=True),
    )(shock_rate, shock_fx, fx_vol, fx_corr, hazard_scale, *(a.reshape(1, count) for a in trades))
    profile, cva = pl.pallas_call(
        hand_out,
        out_shape=(jax.ShapeDtypeStruct((dates, cps), F32), jax.ShapeDtypeStruct((1, cps), F32)),
        in_specs=[vmem(), vmem()],
        out_specs=(anywhere(), anywhere()),
        scratch_shapes=[sems((2,))],
    )(*(pltpu.with_memory_space_constraint(a, pltpu.VMEM) for a in (profile, cva)))
    return profile, cva.reshape(cps)


def solution(mesh):
    placed = (P("tm", "path"), P(None, "tm", "path"), P(), P(), P(), P(), P(), P(), P(), P())
    return jax.shard_map(
        functools.partial(per_device, mesh.shape["tm"], mesh.shape["path"]),
        mesh=mesh,
        in_specs=placed,
        out_specs=(P("tm", None), P()),
        check_vma=False,
    )
```

```python
import functools
import math

import jax
import jax.numpy as jnp
from jax import lax
from jax.experimental import pallas as pl
from jax.experimental.pallas import tpu as pltpu
from jax.sharding import PartitionSpec as P

HORIZON = 5.0
RATE_DOM = 0.03
RATE_FOR = 0.01
LOSS_SHARE = 0.6
RATE_SHIFT = 1.5
LOG2E = 1.4426950408889634

SIZES = (1, 1, 2, 2, 2)
TILE = 256
CROWD = 8
MESH = pl.DeviceIdType.MESH
F32 = jnp.float32
BF16 = jnp.bfloat16


def split3(x):
    high = x.astype(BF16)
    rest = x - high.astype(F32)
    mid = rest.astype(BF16)
    low = (rest - mid.astype(F32)).astype(BF16)
    return high, mid, low


def split2(x):
    high = x.astype(BF16)
    return high, (x - high.astype(F32)).astype(BF16)


def iota(shape, dim):
    return lax.broadcasted_iota(jnp.int32, shape, dim)


def ring_far(i, n):
    return min(i, n - i)


def tm_order(n):
    return sorted(range(1, n), key=lambda i: -(ring_far(i // 4, n // 4) + ring_far(i % 4, 4)))


def path_order(n):
    return sorted(range(1, n), key=lambda i: -ring_far(i, n))


def ones_where(mask):
    return jnp.where(mask, 1.0, 0.0)


def kernel(
    geometry,
    rate_hbm, fx_hbm, vol_hbm, corr_hbm, scale_hbm, cp_hbm, ccy_hbm, mat_hbm, notl_hbm, strike_hbm,
    prof_out, cva_out,
    xr, xf, log_ref, ab_ref, sum_ref, rcv_ref, pre_ref, st_ref,
    m1_ref, m2_ref, lhs_ref, wf_ref, wd_ref, ns_ref, net0_ref, net1_ref, net2_ref, net3_ref, haz0_ref, haz1_ref, haz2_ref, haz3_ref, acc_ref,
    part_ref, parts_rcv, cpart_ref, cparts_rcv,
    vol_s, corr_s, scale_s, cp_ref, ccy_ref, mat_ref, notl_ref, strike_ref,
    in_sem, small_sem, s1_send, s1_recv, s2_send, s2_recv, t_send, t_recv,
):
    n_tm, n_path, paths, dates, cps, ccys, total_dates, total_paths = geometry
    dt = HORIZON / total_dates
    decay = math.exp(-2.0 / total_dates)
    noise = math.sqrt(1.0 - decay * decay)
    width = TILE
    tiles = paths // width
    per_tile = width // 128
    chunks = len(SIZES)
    assert paths == 128 * n_tm * sum(SIZES)
    first = [n_tm * sum(SIZES[:k]) for k in range(chunks + 1)]
    me = lax.axis_index("tm")
    my_path = lax.axis_index("path")

    def load_copies(k):
        lanes = pl.ds(first[k] * 128, (first[k + 1] - first[k]) * 128)
        return (
            pltpu.make_async_copy(rate_hbm.at[:, lanes], xr.at[:, lanes], in_sem.at[0, k]),
            pltpu.make_async_copy(fx_hbm.at[:, :, lanes], xf.at[:, :, lanes], in_sem.at[1, k]),
        )

    small = [
        pltpu.make_async_copy(source, target, small_sem.at[q])
        for q, (source, target) in enumerate(
            zip(
                (vol_hbm, corr_hbm, scale_hbm, cp_hbm, ccy_hbm, mat_hbm, notl_hbm, strike_hbm),
                (vol_s, corr_s, scale_s, cp_ref, ccy_ref, mat_ref, notl_ref, strike_ref),
            )
        )
    ]
    for copy in load_copies(0):
        copy.start()
    for copy in small:
        copy.start()
    for k in range(1, chunks):
        for copy in load_copies(k):
            copy.start()

    barrier = pltpu.get_barrier_semaphore()

    for i in tm_order(n_tm):
        pl.semaphore_signal(barrier, inc=1, device_id={"tm": lax.rem(me + i, n_tm)}, device_id_type=MESH)
    for i in path_order(n_path):
        pl.semaphore_signal(
            barrier, inc=1, device_id={"path": lax.rem(my_path + i, n_path)}, device_id_type=MESH
        )

    small[0].wait()
    small[1].wait()

    r, c = iota((96, 160), 0), iota((96, 160), 1)
    s = c - jnp.where(c >= 80, 80, 0)
    in_ccy, in_date = (s >> 4) - 1, s & 15
    last = jnp.full_like(r, 15)
    out_ccy = jnp.where(r < 64, (r & 31) >> 3, jnp.where((r < 80) | (r == 80), -1, jnp.where(r < 85, r - 81, 9)))
    out_date = jnp.where(r < 64, ((r >> 5) << 3) + (r & 7), jnp.where(r < 80, r - 64, last))
    m1_ref[...] = ones_where((in_ccy == out_ccy) & (in_date <= out_date)).astype(BF16)
    r, c = iota((48, 64), 0), iota((48, 64), 1)
    s = c & 31
    in_kind, in_date = s >> 4, s & 15
    out_kind = jnp.where(r < 32, r >> 4, jnp.where(r == 37, 0, jnp.where(r == 38, 1, 9)))
    out_date = jnp.where(r < 32, r & 15, jnp.full_like(r, 15))
    m2_ref[...] = ones_where((in_kind == out_kind) & (in_date <= out_date)).astype(BF16)

    def vec(ref, j):
        return jnp.full((1, 128), ref[j], F32)

    def wide(v, n):
        return jnp.broadcast_to(v[:, :1], (v.shape[0], n))

    c_rate, c_own, c_drift = [], [], []
    for j in range(ccys):
        vol, corr = vec(vol_s, j), vec(corr_s, j)
        c_rate.append(vol * (LOG2E * math.sqrt(dt)) * corr)
        c_own.append(vol * (LOG2E * math.sqrt(dt)) * jnp.sqrt(1.0 - corr * corr))
        c_drift.append((0.5 * LOG2E * dt) * vol * vol)

    def date_col(n):
        return iota((dates, n), 0).astype(F32)

    log_decay = -2.0 / total_dates

    def walk(k):
        group = (first[k + 1] - first[k]) * 128
        lanes = pl.ds(first[k] * 128, group)
        rate = xr[:, lanes]
        rows = [rate * (noise * jnp.exp(-log_decay * date_col(group)))]
        for j in range(ccys):
            rows.append((wide(c_rate[j], group) * rate + wide(c_own[j], group) * xf[j, :, lanes]) - wide(c_drift[j], group))
        right = jnp.concatenate(split2(jnp.concatenate(rows, axis=0)), axis=0)
        out = jnp.dot(m1_ref[...], right, preferred_element_type=F32)
        power = jnp.exp(log_decay * date_col(group))
        shifted = out[64:80] * power + RATE_SHIFT
        cost = dt * (0.1 + 0.5 * shifted * shifted)
        slope = (dt * decay) * power * shifted
        right = jnp.concatenate(split2(jnp.concatenate([cost, slope], axis=0)), axis=0)
        out2 = jnp.dot(m2_ref[...], right, preferred_element_type=F32)
        row = iota((8, group), 0)
        ends = jnp.where(row == 0, decay ** (dates - 1), 1.0) * out[80:88] + out2[32:40]
        for q in range(group // width):
            part = slice(q * width, (q + 1) * width)
            log_ref[first[k] // per_tile + q] = out[:64, part]
            ab_ref[first[k] // per_tile + q] = out2[:32, part]
        for q in range(group // 128):
            sum_ref[first[k] + q] = ends[:, q * 128 : (q + 1) * 128]

    def columns(k, device):
        return pl.ds(first[k] + device * SIZES[k], SIZES[k])

    def send1(k, i):
        owner = lax.rem(me + i, n_tm)
        return pltpu.make_async_remote_copy(
            src_ref=sum_ref.at[columns(k, owner), pl.ds(0, 7)],
            dst_ref=rcv_ref.at[columns(k, me), pl.ds(0, 7)],
            send_sem=s1_send.at[k],
            recv_sem=s1_recv.at[k],
            device_id={"tm": owner},
            device_id_type=MESH,
        )

    def send2(k, i):
        block = lax.rem(me + i, n_tm)
        return pltpu.make_async_remote_copy(
            src_ref=pre_ref.at[columns(k, block), pl.ds(0, 6)],
            dst_ref=st_ref.at[columns(k, me), pl.ds(0, 6)],
            send_sem=s2_send.at[k],
            recv_sem=s2_recv.at[k],
            device_id={"tm": block},
            device_id_type=MESH,
        )

    def all_of(send, recv, k, rows):
        return pltpu.make_async_remote_copy(
            src_ref=rcv_ref.at[pl.ds(0, (n_tm - 1) * SIZES[k]), pl.ds(0, rows)],
            dst_ref=rcv_ref.at[pl.ds(0, (n_tm - 1) * SIZES[k]), pl.ds(0, rows)],
            send_sem=send.at[k],
            recv_sem=recv.at[k],
            device_id={"tm": me},
            device_id_type=MESH,
        )

    def walk_and_send(k):
        with jax.named_scope(f"inwait{k}"):
            for copy in load_copies(k):
                copy.wait()
        with jax.named_scope(f"walk{k}"):
            walk(k)
        if k == 0:
            with jax.named_scope("barrier"):
                pl.semaphore_wait(barrier, n_tm - 1 + n_path - 1)
        for i in tm_order(n_tm):
            send1(k, i).start()

    block_gain = decay**dates
    block_square = 0.5 * dt * sum(decay ** (2 * (u + 1)) for u in range(dates))
    kind = iota((8, 128), 0)

    def own(k):
        with jax.named_scope(f"wait1_{k}"):
            all_of(s1_send, s1_recv, k, 7).wait_recv()
        rcv_ref[columns(k, me)] = sum_ref[columns(k, me)]
        for q in range(SIZES[k]):
            rate = rest = jnp.zeros((8, 128), F32)
            for b in range(n_tm):
                at = first[k] + b * SIZES[k] + q
                pre_ref[at] = jnp.where(kind == 0, rate, rest)
                if b < n_tm - 1:
                    x = rcv_ref[at]
                    slope = jnp.broadcast_to(x[6:7], (8, 128))
                    rest = rest + (x + jnp.where(kind == 5, rate * (slope + rate * block_square), 0.0))
                    rate = block_gain * rate + jnp.broadcast_to(x[0:1], (8, 128))
        for i in tm_order(n_tm):
            send2(k, i).start()
        st_ref[columns(k, me)] = pre_ref[columns(k, me)]

    for k in range(chunks - 1):
        walk_and_send(k)
    for copy in small[2:]:
        copy.wait()

    cp, ccy, mat = cp_ref[...], ccy_ref[...], mat_ref[...]
    trades = cp.shape[1]
    date = iota((dates, trades), 0) + me * dates
    alive = date < mat
    left = (mat - date).astype(F32) * dt
    notl = notl_ref[...]
    wf_ref[...] = jnp.where(alive, notl * jnp.exp(-RATE_FOR * left), 0.0)
    wd_ref[...] = jnp.where(alive, -(notl * strike_ref[...]) * jnp.exp(-RATE_DOM * left), 0.0)
    member = cp == iota((cps, trades), 0)
    col = iota((256, trades), 0)
    pick = jnp.concatenate(
        [
            ones_where((col < 160) & (ccy == ((col & 31) >> 3))).astype(BF16),
            ones_where((col >= 160) & (col < 163)).astype(BF16),
        ],
        axis=1,
    )
    r, c = iota((256, 256), 0), iota((256, 256), 1)
    keep = (c >= 160) | ((r >> 5) == (c & 7))
    part = c >> 5
    is_high = (part == 0) | (part == 3) | (c == 160)
    is_mid = (part == 1) | (part == 4) | (c == 161)
    for half in range(2):
        blocks = []
        for t in range(half * 8, half * 8 + 8):
            blocks.append(
                jnp.concatenate(
                    [
                        jnp.where(member, wf_ref[t : t + 1], 0.0),
                        jnp.where(member, wd_ref[t : t + 1], 0.0),
                    ],
                    axis=1,
                )
            )
        table = jnp.zeros((256, 256), F32)
        for term in split3(jnp.concatenate(blocks, axis=0)):
            table = table + lax.dot_general(
                term, pick, (((1,), (1,)), ((), ())), preferred_element_type=F32
            )
        high, mid, low = split3(jnp.where(keep, table, 0.0))
        chosen = jnp.where(is_high, high.astype(F32), jnp.where(is_mid, mid.astype(F32), low.astype(F32)))
        lhs_ref[half] = chosen.astype(BF16)[:, :176]

    row = iota((cps, 128), 0)
    ns = jnp.zeros((cps, 128), F32)
    for q in range(cps):
        ns = jnp.where(row == q, scale_s[q] * (-LOG2E), ns)
    for t in range(dates):
        ns_ref[t] = ns
    acc_ref[...] = jnp.zeros_like(acc_ref)

    own(0)
    own(1)
    walk_and_send(chunks - 1)

    for k in range(2, chunks - 1):
        own(k)

    squares = 0.5 * dt * jnp.exp(2 * log_decay) * (1.0 - jnp.exp(2 * log_decay * (date_col(width) + 1.0))) * (
        1.0 / (1.0 - math.exp(2 * log_decay))
    )
    fill = jnp.ones((16, width), BF16)

    nets, hazs = (net0_ref, net1_ref, net2_ref, net3_ref), (haz0_ref, haz1_ref, haz2_ref, haz3_ref)

    def prepare(i, slot):
        state = jnp.concatenate([st_ref[i * per_tile + q] for q in range(per_tile)], axis=1)
        rate, hazard = state[0:1], state[5:6]
        ab = ab_ref[i]
        hazs[slot][...] = hazard + ab[:dates] + rate * (ab[dates:] + rate * squares)
        for half in range(2):
            spots = []
            for j in range(ccys):
                at = half * 32 + j * 8
                spots.append(jnp.exp2(log_ref[i, at : at + 8] + state[1 + j : 2 + j]))
            high, mid = split2(jnp.concatenate(spots, axis=0))
            right = jnp.concatenate([high, high, high, mid, mid, fill], axis=0)
            nets[slot][half] = jnp.dot(lhs_ref[half], right, preferred_element_type=F32)

    def weigh(tiles):
        for g in range(0, cps, CROWD):
            scale = ns_ref[0, g : g + CROWD]
            before = []
            for i, slot in tiles:
                for q in range(width // 128):
                    before.append(jnp.exp2(scale * st_ref[i * per_tile + q, 5:6]))
            for t in range(dates):
                at = (t % 8) * cps + g
                total = None
                n = 0
                for i, slot in tiles:
                    for q in range(width // 128):
                        lanes = slice(q * 128, (q + 1) * 128)
                        now = jnp.exp2(ns_ref[t, g : g + CROWD] * hazs[slot][t : t + 1, lanes])
                        worth = jnp.maximum(nets[slot][t // 8, at : at + CROWD, lanes], 0.0) * (before[n] - now)
                        before[n] = now
                        n += 1
                        total = worth if total is None else total + worth
                acc_ref[t * cps + g : t * cps + g + CROWD] += total

    def wait2(k):
        with jax.named_scope(f"wait2_{k}"):
            all_of(s2_send, s2_recv, k, 6).wait_recv()

    wait2(0)
    prepare(0, 0)
    prepare(1, 1)
    with jax.named_scope("weigh"):

        def step(it):
            i = 4 * it
            prepare(i + 2, 2)
            prepare(i + 3, 3)
            weigh([(i, 0), (i + 1, 1)])
            j = jnp.minimum(i + 4, tiles - 2)
            prepare(j, 0)
            prepare(j + 1, 1)
            weigh([(i + 2, 2), (i + 3, 3)])

        begin = 0
        for k in range(1, chunks + 1):
            end = first[k] // per_tile // 4 - (k < chunks)
            pl.loop(begin, end)(step)
            begin = end
            if k == 2:
                own(chunks - 1)
            if k < chunks:
                wait2(k)

    turned = jnp.sum(jnp.transpose(acc_ref[...]), axis=0, keepdims=True)
    part_ref[...] = turned * (1.0 / (total_paths * dt))
    parts_rcv[my_path] = part_ref[...]

    def send_part(i):
        to = lax.rem(my_path + i, n_path)
        return pltpu.make_async_remote_copy(
            src_ref=part_ref,
            dst_ref=parts_rcv.at[my_path],
            send_sem=t_send.at[0],
            recv_sem=t_recv.at[0],
            device_id={"path": to},
            device_id_type=MESH,
        )

    for i in path_order(n_path):
        send_part(i).start()

    def all_parts(ref, n, at, where):
        return pltpu.make_async_remote_copy(
            src_ref=ref.at[pl.ds(0, n - 1)],
            dst_ref=ref.at[pl.ds(0, n - 1)],
            send_sem=t_send.at[at],
            recv_sem=t_recv.at[at],
            device_id=where,
            device_id_type=MESH,
        )

    lane = iota((1, dates * cps), 1)
    at_date = (lane // cps + me * dates).astype(F32)
    discount = (LOSS_SHARE * dt) * jnp.exp(-RATE_DOM * dt * (at_date + 1.0))
    with jax.named_scope("wait_t1"):
        all_parts(parts_rcv, n_path, 0, {"path": my_path}).wait_recv()
    profile = parts_rcv[0]
    for q in range(1, n_path):
        profile = profile + parts_rcv[q]
    for t in range(dates):
        prof_out[t : t + 1] = profile[:, t * cps : (t + 1) * cps]
    terms = profile * discount
    total = terms[:, :128]
    for q in range(1, dates * cps // 128):
        total = total + terms[:, q * 128 : (q + 1) * 128]
    total = total + pltpu.roll(total, 64, 1)
    total = total + pltpu.roll(total, 32, 1)
    cpart_ref[...] = total
    cparts_rcv[me] = total

    def send_cva(i):
        to = lax.rem(me + i, n_tm)
        return pltpu.make_async_remote_copy(
            src_ref=cpart_ref,
            dst_ref=cparts_rcv.at[me],
            send_sem=t_send.at[1],
            recv_sem=t_recv.at[1],
            device_id={"tm": to},
            device_id_type=MESH,
        )

    for i in tm_order(n_tm):
        send_cva(i).start()

    for k in range(chunks):
        all_of(s1_send, s1_recv, k, 7).wait_send()
        all_of(s2_send, s2_recv, k, 6).wait_send()
    all_parts(parts_rcv, n_path, 0, {"path": my_path}).wait_send()
    with jax.named_scope("wait_t2"):
        all_parts(cparts_rcv, n_tm, 1, {"tm": me}).wait_recv()
    cva = cparts_rcv[0]
    for q in range(1, n_tm):
        cva = cva + cparts_rcv[q]
    cva_out[...] = cva[:, :cps]
    all_parts(cparts_rcv, n_tm, 1, {"tm": me}).wait_send()


def hand_out(profile, cva, profile_out, cva_out, sems):
    copies = [
        pltpu.make_async_copy(profile, profile_out, sems.at[0]),
        pltpu.make_async_copy(cva, cva_out, sems.at[1]),
    ]
    for copy in copies:
        copy.start()
    for copy in copies:
        copy.wait()


def per_device(n_tm, n_path, shock_rate, shock_fx, fx_vol, fx_corr, hazard_scale, *trades):
    dates, paths = shock_rate.shape
    ccys, cps = fx_vol.shape[0], hazard_scale.shape[0]
    geometry = (n_tm, n_path, paths, dates, cps, ccys, dates * n_tm, paths * n_path)
    width = TILE
    tiles, columns, chunks = paths // width, paths // 128, len(SIZES)
    count = trades[0].shape[0]
    vmem = functools.partial(pl.BlockSpec, memory_space=pltpu.VMEM)
    anywhere = functools.partial(pl.BlockSpec, memory_space=pl.ANY)
    sems = pltpu.SemaphoreType.DMA
    profile, cva = pl.pallas_call(
        functools.partial(kernel, geometry),
        out_shape=(
            pltpu.VMEM((dates, cps), F32),
            pltpu.VMEM((1, cps), F32),
        ),
        in_specs=[anywhere()] * 10,
        out_specs=(vmem(), vmem()),
        scratch_shapes=[
            pltpu.VMEM((dates, paths), F32),
            pltpu.VMEM((ccys, dates, paths), F32),
            pltpu.VMEM((tiles, 64, width), F32),
            pltpu.VMEM((tiles, 32, width), F32),
            pltpu.VMEM((columns, 8, 128), F32),
            pltpu.VMEM((columns, 8, 128), F32),
            pltpu.VMEM((columns, 8, 128), F32),
            pltpu.VMEM((columns, 8, 128), F32),
            pltpu.VMEM((96, 160), BF16),
            pltpu.VMEM((48, 64), BF16),
            pltpu.VMEM((2, 256, 176), BF16),
            pltpu.VMEM((dates, count), F32),
            pltpu.VMEM((dates, count), F32),
            pltpu.VMEM((dates, cps, 128), F32),
            pltpu.VMEM((2, 256, width), F32),
            pltpu.VMEM((2, 256, width), F32),
            pltpu.VMEM((2, 256, width), F32),
            pltpu.VMEM((2, 256, width), F32),
            pltpu.VMEM((dates, width), F32),
            pltpu.VMEM((dates, width), F32),
            pltpu.VMEM((dates, width), F32),
            pltpu.VMEM((dates, width), F32),
            pltpu.VMEM((dates * cps, 128), F32),
            pltpu.VMEM((1, dates * cps), F32),
            pltpu.VMEM((n_path, 1, dates * cps), F32),
            pltpu.VMEM((1, 128), F32),
            pltpu.VMEM((n_tm, 1, 128), F32),
            pltpu.SMEM((ccys,), F32),
            pltpu.SMEM((ccys,), F32),
            pltpu.SMEM((cps,), F32),
            pltpu.VMEM((1, count), jnp.int32),
            pltpu.VMEM((1, count), jnp.int32),
            pltpu.VMEM((1, count), jnp.int32),
            pltpu.VMEM((1, count), F32),
            pltpu.VMEM((1, count), F32),
            sems((2, chunks)),
            sems((8,)),
            sems((chunks,)),
            sems((chunks,)),
            sems((chunks,)),
            sems((chunks,)),
            sems((2,)),
            sems((2,)),
        ],
        compiler_params=pltpu.CompilerParams(collective_id=0, has_side_effects=True),
    )(shock_rate, shock_fx, fx_vol, fx_corr, hazard_scale, *(a.reshape(1, count) for a in trades))
    profile, cva = pl.pallas_call(
        hand_out,
        out_shape=(jax.ShapeDtypeStruct((dates, cps), F32), jax.ShapeDtypeStruct((1, cps), F32)),
        in_specs=[vmem(), vmem()],
        out_specs=(anywhere(), anywhere()),
        scratch_shapes=[sems((2,))],
    )(*(pltpu.with_memory_space_constraint(a, pltpu.VMEM) for a in (profile, cva)))
    return profile, cva.reshape(cps)


def solution(mesh):
    placed = (P("tm", "path"), P(None, "tm", "path"), P(), P(), P(), P(), P(), P(), P(), P())
    return jax.shard_map(
        functools.partial(per_device, mesh.shape["tm"], mesh.shape["path"]),
        mesh=mesh,
        in_specs=placed,
        out_specs=(P("tm", None), P()),
        check_vma=False,
    )
```

```python
import functools
import math

import jax
import jax.numpy as jnp
from jax import lax
from jax.experimental import pallas as pl
from jax.experimental.pallas import tpu as pltpu
from jax.sharding import PartitionSpec as P

HORIZON = 5.0
RATE_DOM = 0.03
RATE_FOR = 0.01
LOSS_SHARE = 0.6
RATE_SHIFT = 1.5
LOG2E = 1.4426950408889634

SIZES = (1, 1, 2, 2, 2)
TILE = 256
CROWD = 8
MESH = pl.DeviceIdType.MESH
F32 = jnp.float32
BF16 = jnp.bfloat16


def split3(x):
    high = x.astype(BF16)
    rest = x - high.astype(F32)
    mid = rest.astype(BF16)
    low = (rest - mid.astype(F32)).astype(BF16)
    return high, mid, low


def split2(x):
    high = x.astype(BF16)
    return high, (x - high.astype(F32)).astype(BF16)


def iota(shape, dim):
    return lax.broadcasted_iota(jnp.int32, shape, dim)


def ring_far(i, n):
    return min(i, n - i)


def tm_order(n):
    return sorted(range(1, n), key=lambda i: -(ring_far(i // 4, n // 4) + ring_far(i % 4, 4)))


def path_order(n):
    return sorted(range(1, n), key=lambda i: -ring_far(i, n))


def ones_where(mask):
    return jnp.where(mask, 1.0, 0.0)


def kernel(
    geometry,
    rate_hbm, fx_hbm, vol_hbm, corr_hbm, scale_hbm, cp_hbm, ccy_hbm, mat_hbm, notl_hbm, strike_hbm,
    prof_out, cva_out,
    xr, xf, log_ref, ab_ref, sum_ref, rcv_ref, pre_ref, st_ref,
    m1_ref, m2_ref, lhs_ref, wf_ref, wd_ref, ns_ref, net0_ref, net1_ref, net2_ref, net3_ref, haz0_ref, haz1_ref, haz2_ref, haz3_ref, acc_ref,
    part_ref, parts_rcv, cpart_ref, cparts_rcv,
    vol_s, corr_s, scale_s, cp_ref, ccy_ref, mat_ref, notl_ref, strike_ref,
    in_sem, small_sem, s1_send, s1_recv, s2_send, s2_recv, t_send, t_recv,
):
    n_tm, n_path, paths, dates, cps, ccys, total_dates, total_paths = geometry
    dt = HORIZON / total_dates
    decay = math.exp(-2.0 / total_dates)
    noise = math.sqrt(1.0 - decay * decay)
    width = TILE
    tiles = paths // width
    per_tile = width // 128
    chunks = len(SIZES)
    assert paths == 128 * n_tm * sum(SIZES)
    first = [n_tm * sum(SIZES[:k]) for k in range(chunks + 1)]
    me = lax.axis_index("tm")
    my_path = lax.axis_index("path")
    near = lax.rem(my_path, 2)
    near_path, far_path = my_path + 1 - near, my_path - near

    def load_copies(k):
        lanes = pl.ds(first[k] * 128, (first[k + 1] - first[k]) * 128)
        return (
            pltpu.make_async_copy(rate_hbm.at[:, lanes], xr.at[:, lanes], in_sem.at[0, k]),
            pltpu.make_async_copy(fx_hbm.at[:, :, lanes], xf.at[:, :, lanes], in_sem.at[1, k]),
        )

    small = [
        pltpu.make_async_copy(source, target, small_sem.at[q])
        for q, (source, target) in enumerate(
            zip(
                (vol_hbm, corr_hbm, scale_hbm, cp_hbm, ccy_hbm, mat_hbm, notl_hbm, strike_hbm),
                (vol_s, corr_s, scale_s, cp_ref, ccy_ref, mat_ref, notl_ref, strike_ref),
            )
        )
    ]
    for copy in load_copies(0):
        copy.start()
    for copy in small:
        copy.start()
    for k in range(1, chunks):
        for copy in load_copies(k):
            copy.start()

    barrier = pltpu.get_barrier_semaphore()

    for i in tm_order(n_tm):
        pl.semaphore_signal(barrier, inc=1, device_id={"tm": lax.rem(me + i, n_tm)}, device_id_type=MESH)
        pl.semaphore_signal(
            barrier,
            inc=1,
            device_id={"tm": lax.rem(me + i, n_tm), "path": near_path + far_path - my_path},
            device_id_type=MESH,
        )
    for i in path_order(n_path):
        pl.semaphore_signal(
            barrier, inc=1, device_id={"path": lax.rem(my_path + i, n_path)}, device_id_type=MESH
        )

    small[0].wait()
    small[1].wait()

    r, c = iota((96, 160), 0), iota((96, 160), 1)
    s = c - jnp.where(c >= 80, 80, 0)
    in_ccy, in_date = (s >> 4) - 1, s & 15
    last = jnp.full_like(r, 15)
    out_ccy = jnp.where(r < 64, (r & 31) >> 3, jnp.where((r < 80) | (r == 80), -1, jnp.where(r < 85, r - 81, 9)))
    out_date = jnp.where(r < 64, ((r >> 5) << 3) + (r & 7), jnp.where(r < 80, r - 64, last))
    m1_ref[...] = ones_where((in_ccy == out_ccy) & (in_date <= out_date)).astype(BF16)
    r, c = iota((48, 64), 0), iota((48, 64), 1)
    s = c & 31
    in_kind, in_date = s >> 4, s & 15
    out_kind = jnp.where(r < 32, r >> 4, jnp.where(r == 37, 0, jnp.where(r == 38, 1, 9)))
    out_date = jnp.where(r < 32, r & 15, jnp.full_like(r, 15))
    m2_ref[...] = ones_where((in_kind == out_kind) & (in_date <= out_date)).astype(BF16)

    def vec(ref, j):
        return jnp.full((1, 128), ref[j], F32)

    def wide(v, n):
        return jnp.broadcast_to(v[:, :1], (v.shape[0], n))

    c_rate, c_own, c_drift = [], [], []
    for j in range(ccys):
        vol, corr = vec(vol_s, j), vec(corr_s, j)
        c_rate.append(vol * (LOG2E * math.sqrt(dt)) * corr)
        c_own.append(vol * (LOG2E * math.sqrt(dt)) * jnp.sqrt(1.0 - corr * corr))
        c_drift.append((0.5 * LOG2E * dt) * vol * vol)

    def date_col(n):
        return iota((dates, n), 0).astype(F32)

    log_decay = -2.0 / total_dates

    def walk(k):
        group = (first[k + 1] - first[k]) * 128
        lanes = pl.ds(first[k] * 128, group)
        rate = xr[:, lanes]
        rows = [rate * (noise * jnp.exp(-log_decay * date_col(group)))]
        for j in range(ccys):
            rows.append((wide(c_rate[j], group) * rate + wide(c_own[j], group) * xf[j, :, lanes]) - wide(c_drift[j], group))
        right = jnp.concatenate(split2(jnp.concatenate(rows, axis=0)), axis=0)
        out = jnp.dot(m1_ref[...], right, preferred_element_type=F32)
        power = jnp.exp(log_decay * date_col(group))
        shifted = out[64:80] * power + RATE_SHIFT
        cost = dt * (0.1 + 0.5 * shifted * shifted)
        slope = (dt * decay) * power * shifted
        right = jnp.concatenate(split2(jnp.concatenate([cost, slope], axis=0)), axis=0)
        out2 = jnp.dot(m2_ref[...], right, preferred_element_type=F32)
        row = iota((8, group), 0)
        ends = jnp.where(row == 0, decay ** (dates - 1), 1.0) * out[80:88] + out2[32:40]
        for q in range(group // width):
            part = slice(q * width, (q + 1) * width)
            log_ref[first[k] // per_tile + q] = out[:64, part]
            ab_ref[first[k] // per_tile + q] = out2[:32, part]
        for q in range(group // 128):
            sum_ref[first[k] + q] = ends[:, q * 128 : (q + 1) * 128]

    def columns(k, device):
        return pl.ds(first[k] + device * SIZES[k], SIZES[k])

    def send1(k, i):
        owner = lax.rem(me + i, n_tm)
        return pltpu.make_async_remote_copy(
            src_ref=sum_ref.at[columns(k, owner), pl.ds(0, 7)],
            dst_ref=rcv_ref.at[near, columns(k, me), pl.ds(0, 7)],
            send_sem=s1_send.at[k],
            recv_sem=s1_recv.at[near, k],
            device_id={"tm": owner, "path": near_path},
            device_id_type=MESH,
        )

    def send2(core, k, i):
        block = lax.rem(me + i, n_tm)
        return pltpu.make_async_remote_copy(
            src_ref=pre_ref.at[core, columns(k, block), pl.ds(0, 6)],
            dst_ref=st_ref.at[columns(k, me), pl.ds(0, 6)],
            send_sem=s2_send.at[core, k],
            recv_sem=s2_recv.at[k],
            device_id={"tm": block, "path": far_path + core},
            device_id_type=MESH,
        )

    def all_of(send, recv, k, rows, count):
        part = rcv_ref.at[0, pl.ds(0, count * SIZES[k]), pl.ds(0, rows)]
        return pltpu.make_async_remote_copy(
            src_ref=part, dst_ref=part, send_sem=send, recv_sem=recv, device_id={"tm": me}, device_id_type=MESH
        )

    def each_core(act):
        pl.when(near == 1)(lambda: act(n_tm - 1))
        pl.when(near == 0)(lambda: act(n_tm))

    def walk_and_send(k):
        with jax.named_scope(f"inwait{k}"):
            for copy in load_copies(k):
                copy.wait()
        with jax.named_scope(f"walk{k}"):
            walk(k)
        if k == 0:
            with jax.named_scope("barrier"):
                pl.semaphore_wait(barrier, 2 * (n_tm - 1) + n_path - 1)
        for i in tm_order(n_tm):
            send1(k, i).start()

        @pl.when(near == 0)
        def _():
            send1(k, 0).start()

    block_gain = decay**dates
    block_square = 0.5 * dt * sum(decay ** (2 * (u + 1)) for u in range(dates))
    kind = iota((8, 128), 0)

    def order(core, k):
        for q in range(SIZES[k]):
            rate = rest = jnp.zeros((8, 128), F32)
            for b in range(n_tm):
                at = first[k] + b * SIZES[k] + q
                pre_ref[core, at] = jnp.where(kind == 0, rate, rest)
                if b < n_tm - 1:
                    x = rcv_ref[core, at]
                    slope = jnp.broadcast_to(x[6:7], (8, 128))
                    rest = rest + (x + jnp.where(kind == 5, rate * (slope + rate * block_square), 0.0))
                    rate = block_gain * rate + jnp.broadcast_to(x[0:1], (8, 128))

    def own(k):
        @pl.when(near == 1)
        def _():
            with jax.named_scope(f"wait1_{k}"):
                all_of(s1_send.at[k], s1_recv.at[0, k], k, 7, n_tm).wait_recv()
            order(0, k)
            for i in tm_order(n_tm) + [0]:
                send2(0, k, i).start()
            all_of(s1_send.at[k], s1_recv.at[1, k], k, 7, n_tm - 1).wait_recv()
            rcv_ref[1, columns(k, me)] = sum_ref[columns(k, me)]
            order(1, k)
            for i in tm_order(n_tm):
                send2(1, k, i).start()
            st_ref[columns(k, me)] = pre_ref[1, columns(k, me)]

    for k in range(chunks - 1):
        walk_and_send(k)
    for copy in small[2:]:
        copy.wait()

    cp, ccy, mat = cp_ref[...], ccy_ref[...], mat_ref[...]
    trades = cp.shape[1]
    date = iota((dates, trades), 0) + me * dates
    alive = date < mat
    left = (mat - date).astype(F32) * dt
    notl = notl_ref[...]
    wf_ref[...] = jnp.where(alive, notl * jnp.exp(-RATE_FOR * left), 0.0)
    wd_ref[...] = jnp.where(alive, -(notl * strike_ref[...]) * jnp.exp(-RATE_DOM * left), 0.0)
    member = cp == iota((cps, trades), 0)
    col = iota((256, trades), 0)
    pick = jnp.concatenate(
        [
            ones_where((col < 160) & (ccy == ((col & 31) >> 3))).astype(BF16),
            ones_where((col >= 160) & (col < 163)).astype(BF16),
        ],
        axis=1,
    )
    r, c = iota((256, 256), 0), iota((256, 256), 1)
    keep = (c >= 160) | ((r >> 5) == (c & 7))
    part = c >> 5
    is_high = (part == 0) | (part == 3) | (c == 160)
    is_mid = (part == 1) | (part == 4) | (c == 161)
    for half in range(2):
        blocks = []
        for t in range(half * 8, half * 8 + 8):
            blocks.append(
                jnp.concatenate(
                    [
                        jnp.where(member, wf_ref[t : t + 1], 0.0),
                        jnp.where(member, wd_ref[t : t + 1], 0.0),
                    ],
                    axis=1,
                )
            )
        table = jnp.zeros((256, 256), F32)
        for term in split3(jnp.concatenate(blocks, axis=0)):
            table = table + lax.dot_general(
                term, pick, (((1,), (1,)), ((), ())), preferred_element_type=F32
            )
        high, mid, low = split3(jnp.where(keep, table, 0.0))
        chosen = jnp.where(is_high, high.astype(F32), jnp.where(is_mid, mid.astype(F32), low.astype(F32)))
        lhs_ref[half] = chosen.astype(BF16)[:, :176]

    row = iota((cps, 128), 0)
    ns = jnp.zeros((cps, 128), F32)
    for q in range(cps):
        ns = jnp.where(row == q, scale_s[q] * (-LOG2E), ns)
    for t in range(dates):
        ns_ref[t] = ns
    acc_ref[...] = jnp.zeros_like(acc_ref)

    own(0)
    own(1)
    walk_and_send(chunks - 1)

    for k in range(2, chunks - 1):
        own(k)

    squares = 0.5 * dt * jnp.exp(2 * log_decay) * (1.0 - jnp.exp(2 * log_decay * (date_col(width) + 1.0))) * (
        1.0 / (1.0 - math.exp(2 * log_decay))
    )
    fill = jnp.ones((16, width), BF16)

    nets, hazs = (net0_ref, net1_ref, net2_ref, net3_ref), (haz0_ref, haz1_ref, haz2_ref, haz3_ref)

    def prepare(i, slot):
        state = jnp.concatenate([st_ref[i * per_tile + q] for q in range(per_tile)], axis=1)
        rate, hazard = state[0:1], state[5:6]
        ab = ab_ref[i]
        hazs[slot][...] = hazard + ab[:dates] + rate * (ab[dates:] + rate * squares)
        for half in range(2):
            spots = []
            for j in range(ccys):
                at = half * 32 + j * 8
                spots.append(jnp.exp2(log_ref[i, at : at + 8] + state[1 + j : 2 + j]))
            high, mid = split2(jnp.concatenate(spots, axis=0))
            right = jnp.concatenate([high, high, high, mid, mid, fill], axis=0)
            nets[slot][half] = jnp.dot(lhs_ref[half], right, preferred_element_type=F32)

    def weigh(tiles):
        for g in range(0, cps, CROWD):
            scale = ns_ref[0, g : g + CROWD]
            before = []
            for i, slot in tiles:
                for q in range(width // 128):
                    before.append(jnp.exp2(scale * st_ref[i * per_tile + q, 5:6]))
            for t in range(dates):
                at = (t % 8) * cps + g
                total = None
                n = 0
                for i, slot in tiles:
                    for q in range(width // 128):
                        lanes = slice(q * 128, (q + 1) * 128)
                        now = jnp.exp2(ns_ref[t, g : g + CROWD] * hazs[slot][t : t + 1, lanes])
                        worth = jnp.maximum(nets[slot][t // 8, at : at + CROWD, lanes], 0.0) * (before[n] - now)
                        before[n] = now
                        n += 1
                        total = worth if total is None else total + worth
                acc_ref[t * cps + g : t * cps + g + CROWD] += total

    def wait2(k):
        with jax.named_scope(f"wait2_{k}"):
            each_core(lambda n: all_of(s1_send.at[k], s2_recv.at[k], k, 6, n).wait_recv())

    wait2(0)
    prepare(0, 0)
    prepare(1, 1)
    with jax.named_scope("weigh"):

        def step(it):
            i = 4 * it
            prepare(i + 2, 2)
            prepare(i + 3, 3)
            weigh([(i, 0), (i + 1, 1)])
            j = jnp.minimum(i + 4, tiles - 2)
            prepare(j, 0)
            prepare(j + 1, 1)
            weigh([(i + 2, 2), (i + 3, 3)])

        begin = 0
        for k in range(1, chunks + 1):
            end = first[k] // per_tile // 4 - (k < chunks)
            pl.loop(begin, end)(step)
            begin = end
            if k == 2:
                own(chunks - 1)
            if k < chunks:
                wait2(k)

    turned = jnp.sum(jnp.transpose(acc_ref[...]), axis=0, keepdims=True)
    part_ref[...] = turned * (1.0 / (total_paths * dt))
    parts_rcv[my_path] = part_ref[...]

    def send_part(i):
        to = lax.rem(my_path + i, n_path)
        return pltpu.make_async_remote_copy(
            src_ref=part_ref,
            dst_ref=parts_rcv.at[my_path],
            send_sem=t_send.at[0],
            recv_sem=t_recv.at[0],
            device_id={"path": to},
            device_id_type=MESH,
        )

    for i in path_order(n_path):
        send_part(i).start()

    def all_parts(ref, n, at, where):
        return pltpu.make_async_remote_copy(
            src_ref=ref.at[pl.ds(0, n - 1)],
            dst_ref=ref.at[pl.ds(0, n - 1)],
            send_sem=t_send.at[at],
            recv_sem=t_recv.at[at],
            device_id=where,
            device_id_type=MESH,
        )

    lane = iota((1, dates * cps), 1)
    at_date = (lane // cps + me * dates).astype(F32)
    discount = (LOSS_SHARE * dt) * jnp.exp(-RATE_DOM * dt * (at_date + 1.0))
    with jax.named_scope("wait_t1"):
        all_parts(parts_rcv, n_path, 0, {"path": my_path}).wait_recv()
    profile = parts_rcv[0]
    for q in range(1, n_path):
        profile = profile + parts_rcv[q]
    for t in range(dates):
        prof_out[t : t + 1] = profile[:, t * cps : (t + 1) * cps]
    terms = profile * discount
    total = terms[:, :128]
    for q in range(1, dates * cps // 128):
        total = total + terms[:, q * 128 : (q + 1) * 128]
    total = total + pltpu.roll(total, 64, 1)
    total = total + pltpu.roll(total, 32, 1)
    cpart_ref[...] = total
    cparts_rcv[me] = total

    def send_cva(core, i):
        to = lax.rem(me + i, n_tm)
        return pltpu.make_async_remote_copy(
            src_ref=cpart_ref,
            dst_ref=cparts_rcv.at[me],
            send_sem=t_send.at[1],
            recv_sem=t_recv.at[1],
            device_id={"tm": to, "path": far_path + core},
            device_id_type=MESH,
        )

    @pl.when(near == 1)
    def _():
        for i in tm_order(n_tm):
            send_cva(0, i).start()
            send_cva(1, i).start()


    for k in range(chunks):
        each_core(lambda n: all_of(s1_send.at[k], s1_recv.at[0, k], k, 7, n).wait_send())

        @pl.when(near == 1)
        def _():
            all_of(s2_send.at[0, k], s1_recv.at[0, k], k, 6, n_tm).wait_send()
            all_of(s2_send.at[1, k], s1_recv.at[0, k], k, 6, n_tm - 1).wait_send()

    all_parts(parts_rcv, n_path, 0, {"path": my_path}).wait_send()
    with jax.named_scope("wait_t2"):
        all_parts(cparts_rcv, n_tm, 1, {"tm": me}).wait_recv()
    cva = cparts_rcv[0]
    for q in range(1, n_tm):
        cva = cva + cparts_rcv[q]
    cva_out[...] = cva[:, :cps]

    @pl.when(near == 1)
    def _():
        all_parts(cparts_rcv, n_tm, 1, {"tm": me}).wait_send()
        all_parts(cparts_rcv, n_tm, 1, {"tm": me}).wait_send()


def hand_out(profile, cva, profile_out, cva_out, sems):
    copies = [
        pltpu.make_async_copy(profile, profile_out, sems.at[0]),
        pltpu.make_async_copy(cva, cva_out, sems.at[1]),
    ]
    for copy in copies:
        copy.start()
    for copy in copies:
        copy.wait()


def per_device(n_tm, n_path, shock_rate, shock_fx, fx_vol, fx_corr, hazard_scale, *trades):
    dates, paths = shock_rate.shape
    ccys, cps = fx_vol.shape[0], hazard_scale.shape[0]
    geometry = (n_tm, n_path, paths, dates, cps, ccys, dates * n_tm, paths * n_path)
    width = TILE
    tiles, columns, chunks = paths // width, paths // 128, len(SIZES)
    count = trades[0].shape[0]
    vmem = functools.partial(pl.BlockSpec, memory_space=pltpu.VMEM)
    anywhere = functools.partial(pl.BlockSpec, memory_space=pl.ANY)
    sems = pltpu.SemaphoreType.DMA
    profile, cva = pl.pallas_call(
        functools.partial(kernel, geometry),
        out_shape=(
            pltpu.VMEM((dates, cps), F32),
            pltpu.VMEM((1, cps), F32),
        ),
        in_specs=[anywhere()] * 10,
        out_specs=(vmem(), vmem()),
        scratch_shapes=[
            pltpu.VMEM((dates, paths), F32),
            pltpu.VMEM((ccys, dates, paths), F32),
            pltpu.VMEM((tiles, 64, width), F32),
            pltpu.VMEM((tiles, 32, width), F32),
            pltpu.VMEM((columns, 8, 128), F32),
            pltpu.VMEM((2, columns, 8, 128), F32),
            pltpu.VMEM((2, columns, 8, 128), F32),
            pltpu.VMEM((columns, 8, 128), F32),
            pltpu.VMEM((96, 160), BF16),
            pltpu.VMEM((48, 64), BF16),
            pltpu.VMEM((2, 256, 176), BF16),
            pltpu.VMEM((dates, count), F32),
            pltpu.VMEM((dates, count), F32),
            pltpu.VMEM((dates, cps, 128), F32),
            pltpu.VMEM((2, 256, width), F32),
            pltpu.VMEM((2, 256, width), F32),
            pltpu.VMEM((2, 256, width), F32),
            pltpu.VMEM((2, 256, width), F32),
            pltpu.VMEM((dates, width), F32),
            pltpu.VMEM((dates, width), F32),
            pltpu.VMEM((dates, width), F32),
            pltpu.VMEM((dates, width), F32),
            pltpu.VMEM((dates * cps, 128), F32),
            pltpu.VMEM((1, dates * cps), F32),
            pltpu.VMEM((n_path, 1, dates * cps), F32),
            pltpu.VMEM((1, 128), F32),
            pltpu.VMEM((n_tm, 1, 128), F32),
            pltpu.SMEM((ccys,), F32),
            pltpu.SMEM((ccys,), F32),
            pltpu.SMEM((cps,), F32),
            pltpu.VMEM((1, count), jnp.int32),
            pltpu.VMEM((1, count), jnp.int32),
            pltpu.VMEM((1, count), jnp.int32),
            pltpu.VMEM((1, count), F32),
            pltpu.VMEM((1, count), F32),
            sems((2, chunks)),
            sems((8,)),
            sems((chunks,)),
            sems((2, chunks)),
            sems((2, chunks)),
            sems((chunks,)),
            sems((2,)),
            sems((2,)),
        ],
        compiler_params=pltpu.CompilerParams(collective_id=0, has_side_effects=True),
    )(shock_rate, shock_fx, fx_vol, fx_corr, hazard_scale, *(a.reshape(1, count) for a in trades))
    profile, cva = pl.pallas_call(
        hand_out,
        out_shape=(jax.ShapeDtypeStruct((dates, cps), F32), jax.ShapeDtypeStruct((1, cps), F32)),
        in_specs=[vmem(), vmem()],
        out_specs=(anywhere(), anywhere()),
        scratch_shapes=[sems((2,))],
    )(*(pltpu.with_memory_space_constraint(a, pltpu.VMEM) for a in (profile, cva)))
    return profile, cva.reshape(cps)


def solution(mesh):
    placed = (P("tm", "path"), P(None, "tm", "path"), P(), P(), P(), P(), P(), P(), P(), P())
    return jax.shard_map(
        functools.partial(per_device, mesh.shape["tm"], mesh.shape["path"]),
        mesh=mesh,
        in_specs=placed,
        out_specs=(P("tm", None), P()),
        check_vma=False,
    )
```

```python
import functools
import math

import jax
import jax.numpy as jnp
from jax import lax
from jax.experimental import pallas as pl
from jax.experimental.pallas import tpu as pltpu
from jax.sharding import PartitionSpec as P

HORIZON = 5.0
RATE_DOM = 0.03
RATE_FOR = 0.01
LOSS_SHARE = 0.6
RATE_SHIFT = 1.5
LOG2E = 1.4426950408889634

SIZES = (1, 1, 2, 2, 2)
TILE = 256
CROWD = 8
MESH = pl.DeviceIdType.MESH
F32 = jnp.float32
BF16 = jnp.bfloat16


def split3(x):
    high = x.astype(BF16)
    rest = x - high.astype(F32)
    mid = rest.astype(BF16)
    low = (rest - mid.astype(F32)).astype(BF16)
    return high, mid, low


def split2(x):
    high = x.astype(BF16)
    return high, (x - high.astype(F32)).astype(BF16)


def iota(shape, dim):
    return lax.broadcasted_iota(jnp.int32, shape, dim)


def ring_far(i, n):
    return min(i, n - i)


def tm_order(n):
    return sorted(range(1, n), key=lambda i: -(ring_far(i // 4, n // 4) + ring_far(i % 4, 4)))


def path_order(n):
    return sorted(range(1, n), key=lambda i: -ring_far(i, n))


def ones_where(mask):
    return jnp.where(mask, 1.0, 0.0)


def kernel(
    geometry,
    rate_hbm, fx_hbm, vol_hbm, corr_hbm, scale_hbm, cp_hbm, ccy_hbm, mat_hbm, notl_hbm, strike_hbm,
    prof_out, cva_out,
    xr, xf, log_ref, ab_ref, sum_ref, rcv_ref, pre_ref, st_ref,
    m1_ref, m2_ref, lhs_ref, wf_ref, wd_ref, ns_ref, net0_ref, net1_ref, net2_ref, net3_ref, haz0_ref, haz1_ref, haz2_ref, haz3_ref, acc_ref,
    part_ref, parts_rcv, cpart_ref, cparts_rcv,
    vol_s, corr_s, scale_s, cp_ref, ccy_ref, mat_ref, notl_ref, strike_ref,
    in_sem, small_sem, s1_send, s1_recv, s2_send, s2_recv, t_send, t_recv,
):
    n_tm, n_path, paths, dates, cps, ccys, total_dates, total_paths = geometry
    dt = HORIZON / total_dates
    decay = math.exp(-2.0 / total_dates)
    noise = math.sqrt(1.0 - decay * decay)
    width = TILE
    tiles = paths // width
    per_tile = width // 128
    chunks = len(SIZES)
    assert paths == 128 * n_tm * sum(SIZES)
    first = [n_tm * sum(SIZES[:k]) for k in range(chunks + 1)]
    me = lax.axis_index("tm")
    my_path = lax.axis_index("path")
    near = lax.rem(my_path, 2)
    near_path, far_path = my_path + 1 - near, my_path - near

    def load_copies(k):
        lanes = pl.ds(first[k] * 128, (first[k + 1] - first[k]) * 128)
        return (
            pltpu.make_async_copy(rate_hbm.at[:, lanes], xr.at[:, lanes], in_sem.at[0, k]),
            pltpu.make_async_copy(fx_hbm.at[:, :, lanes], xf.at[:, :, lanes], in_sem.at[1, k]),
        )

    small = [
        pltpu.make_async_copy(source, target, small_sem.at[q])
        for q, (source, target) in enumerate(
            zip(
                (vol_hbm, corr_hbm, scale_hbm, cp_hbm, ccy_hbm, mat_hbm, notl_hbm, strike_hbm),
                (vol_s, corr_s, scale_s, cp_ref, ccy_ref, mat_ref, notl_ref, strike_ref),
            )
        )
    ]
    for copy in load_copies(0):
        copy.start()
    for copy in small:
        copy.start()
    for k in range(1, chunks):
        for copy in load_copies(k):
            copy.start()

    barrier = pltpu.get_barrier_semaphore()

    for i in tm_order(n_tm):
        pl.semaphore_signal(barrier, inc=1, device_id={"tm": ((me + i) & (n_tm - 1))}, device_id_type=MESH)
        pl.semaphore_signal(
            barrier,
            inc=1,
            device_id={"tm": ((me + i) & (n_tm - 1)), "path": near_path + far_path - my_path},
            device_id_type=MESH,
        )
    for i in path_order(n_path):
        pl.semaphore_signal(
            barrier, inc=1, device_id={"path": ((my_path + i) & (n_path - 1))}, device_id_type=MESH
        )

    small[0].wait()
    small[1].wait()

    r, c = iota((96, 160), 0), iota((96, 160), 1)
    s = c - jnp.where(c >= 80, 80, 0)
    in_ccy, in_date = (s >> 4) - 1, s & 15
    last = jnp.full_like(r, 15)
    out_ccy = jnp.where(r < 64, (r & 31) >> 3, jnp.where((r < 80) | (r == 80), -1, jnp.where(r < 85, r - 81, 9)))
    out_date = jnp.where(r < 64, ((r >> 5) << 3) + (r & 7), jnp.where(r < 80, r - 64, last))
    m1_ref[...] = ones_where((in_ccy == out_ccy) & (in_date <= out_date)).astype(BF16)
    r, c = iota((48, 64), 0), iota((48, 64), 1)
    s = c & 31
    in_kind, in_date = s >> 4, s & 15
    out_kind = jnp.where(r < 32, r >> 4, jnp.where(r == 37, 0, jnp.where(r == 38, 1, 9)))
    out_date = jnp.where(r < 32, r & 15, jnp.full_like(r, 15))
    m2_ref[...] = ones_where((in_kind == out_kind) & (in_date <= out_date)).astype(BF16)

    def vec(ref, j):
        return jnp.full((1, 128), ref[j], F32)

    def wide(v, n):
        return jnp.broadcast_to(v[:, :1], (v.shape[0], n))

    c_rate, c_own, c_drift = [], [], []
    for j in range(ccys):
        vol, corr = vec(vol_s, j), vec(corr_s, j)
        c_rate.append(vol * (LOG2E * math.sqrt(dt)) * corr)
        c_own.append(vol * (LOG2E * math.sqrt(dt)) * jnp.sqrt(1.0 - corr * corr))
        c_drift.append((0.5 * LOG2E * dt) * vol * vol)

    def date_col(n):
        return iota((dates, n), 0).astype(F32)

    log_decay = -2.0 / total_dates

    def walk(k):
        group = (first[k + 1] - first[k]) * 128
        lanes = pl.ds(first[k] * 128, group)
        rate = xr[:, lanes]
        rows = [rate * (noise * jnp.exp(-log_decay * date_col(group)))]
        for j in range(ccys):
            rows.append((wide(c_rate[j], group) * rate + wide(c_own[j], group) * xf[j, :, lanes]) - wide(c_drift[j], group))
        right = jnp.concatenate(split2(jnp.concatenate(rows, axis=0)), axis=0)
        out = jnp.dot(m1_ref[...], right, preferred_element_type=F32)
        power = jnp.exp(log_decay * date_col(group))
        shifted = out[64:80] * power + RATE_SHIFT
        cost = dt * (0.1 + 0.5 * shifted * shifted)
        slope = (dt * decay) * power * shifted
        right = jnp.concatenate(split2(jnp.concatenate([cost, slope], axis=0)), axis=0)
        out2 = jnp.dot(m2_ref[...], right, preferred_element_type=F32)
        row = iota((8, group), 0)
        ends = jnp.where(row == 0, decay ** (dates - 1), 1.0) * out[80:88] + out2[32:40]
        for q in range(group // width):
            part = slice(q * width, (q + 1) * width)
            log_ref[first[k] // per_tile + q] = out[:64, part]
            ab_ref[first[k] // per_tile + q] = out2[:32, part]
        for q in range(group // 128):
            sum_ref[first[k] + q] = ends[:, q * 128 : (q + 1) * 128]

    def columns(k, device):
        return pl.ds(first[k] + device * SIZES[k], SIZES[k])

    def send1(k, i):
        owner = ((me + i) & (n_tm - 1))
        return pltpu.make_async_remote_copy(
            src_ref=sum_ref.at[columns(k, owner), pl.ds(0, 7)],
            dst_ref=rcv_ref.at[near, columns(k, me), pl.ds(0, 7)],
            send_sem=s1_send.at[k],
            recv_sem=s1_recv.at[near, k],
            device_id={"tm": owner, "path": near_path},
            device_id_type=MESH,
        )

    def send2(core, k, i):
        block = ((me + i) & (n_tm - 1))
        return pltpu.make_async_remote_copy(
            src_ref=pre_ref.at[core, columns(k, block), pl.ds(0, 6)],
            dst_ref=st_ref.at[columns(k, me), pl.ds(0, 6)],
            send_sem=s2_send.at[core, k],
            recv_sem=s2_recv.at[k],
            device_id={"tm": block, "path": far_path + core},
            device_id_type=MESH,
        )

    def all_of(send, recv, k, rows, count):
        part = rcv_ref.at[0, pl.ds(0, count * SIZES[k]), pl.ds(0, rows)]
        return pltpu.make_async_remote_copy(
            src_ref=part, dst_ref=part, send_sem=send, recv_sem=recv, device_id={"tm": me}, device_id_type=MESH
        )

    def each_core(act):
        pl.when(near == 1)(lambda: act(n_tm - 1))
        pl.when(near == 0)(lambda: act(n_tm))

    def walk_and_send(k):
        with jax.named_scope(f"inwait{k}"):
            for copy in load_copies(k):
                copy.wait()
        with jax.named_scope(f"walk{k}"):
            walk(k)
        if k == 0:
            with jax.named_scope("barrier"):
                pl.semaphore_wait(barrier, 2 * (n_tm - 1) + n_path - 1)
        for i in tm_order(n_tm):
            send1(k, i).start()

        @pl.when(near == 0)
        def _():
            send1(k, 0).start()

    block_gain = decay**dates
    block_square = 0.5 * dt * sum(decay ** (2 * (u + 1)) for u in range(dates))
    kind = iota((8, 128), 0)

    def order(core, k):
        for q in range(SIZES[k]):
            rate = rest = jnp.zeros((8, 128), F32)
            for b in range(n_tm):
                at = first[k] + b * SIZES[k] + q
                pre_ref[core, at] = jnp.where(kind == 0, rate, rest)
                if b < n_tm - 1:
                    x = rcv_ref[core, at]
                    slope = jnp.broadcast_to(x[6:7], (8, 128))
                    rest = rest + (x + jnp.where(kind == 5, rate * (slope + rate * block_square), 0.0))
                    rate = block_gain * rate + jnp.broadcast_to(x[0:1], (8, 128))

    def own(k):
        @pl.when(near == 1)
        def _():
            with jax.named_scope(f"wait1_{k}"):
                all_of(s1_send.at[k], s1_recv.at[0, k], k, 7, n_tm).wait_recv()
            order(0, k)
            for i in tm_order(n_tm) + [0]:
                send2(0, k, i).start()
            all_of(s1_send.at[k], s1_recv.at[1, k], k, 7, n_tm - 1).wait_recv()
            rcv_ref[1, columns(k, me)] = sum_ref[columns(k, me)]
            order(1, k)
            for i in tm_order(n_tm):
                send2(1, k, i).start()
            st_ref[columns(k, me)] = pre_ref[1, columns(k, me)]

    for k in range(chunks - 1):
        walk_and_send(k)
    for copy in small[2:]:
        copy.wait()

    cp, ccy, mat = cp_ref[...], ccy_ref[...], mat_ref[...]
    trades = cp.shape[1]
    date = iota((dates, trades), 0) + me * dates
    alive = date < mat
    left = (mat - date).astype(F32) * dt
    notl = notl_ref[...]
    wf_ref[...] = jnp.where(alive, notl * jnp.exp(-RATE_FOR * left), 0.0)
    wd_ref[...] = jnp.where(alive, -(notl * strike_ref[...]) * jnp.exp(-RATE_DOM * left), 0.0)
    member = cp == iota((cps, trades), 0)
    col = iota((256, trades), 0)
    pick = jnp.concatenate(
        [
            ones_where((col < 160) & (ccy == ((col & 31) >> 3))).astype(BF16),
            ones_where((col >= 160) & (col < 163)).astype(BF16),
        ],
        axis=1,
    )
    r, c = iota((256, 256), 0), iota((256, 256), 1)
    keep = (c >= 160) | ((r >> 5) == (c & 7))
    part = c >> 5
    is_high = (part == 0) | (part == 3) | (c == 160)
    is_mid = (part == 1) | (part == 4) | (c == 161)
    for half in range(2):
        blocks = []
        for t in range(half * 8, half * 8 + 8):
            blocks.append(
                jnp.concatenate(
                    [
                        jnp.where(member, wf_ref[t : t + 1], 0.0),
                        jnp.where(member, wd_ref[t : t + 1], 0.0),
                    ],
                    axis=1,
                )
            )
        table = jnp.zeros((256, 256), F32)
        for term in split3(jnp.concatenate(blocks, axis=0)):
            table = table + lax.dot_general(
                term, pick, (((1,), (1,)), ((), ())), preferred_element_type=F32
            )
        high, mid, low = split3(jnp.where(keep, table, 0.0))
        chosen = jnp.where(is_high, high.astype(F32), jnp.where(is_mid, mid.astype(F32), low.astype(F32)))
        lhs_ref[half] = chosen.astype(BF16)[:, :176]

    row = iota((cps, 128), 0)
    ns = jnp.zeros((cps, 128), F32)
    for q in range(cps):
        ns = jnp.where(row == q, scale_s[q] * (-LOG2E), ns)
    for t in range(dates):
        ns_ref[t] = ns
    acc_ref[...] = jnp.zeros_like(acc_ref)

    own(0)
    own(1)
    walk_and_send(chunks - 1)

    for k in range(2, chunks - 1):
        own(k)

    squares = 0.5 * dt * jnp.exp(2 * log_decay) * (1.0 - jnp.exp(2 * log_decay * (date_col(width) + 1.0))) * (
        1.0 / (1.0 - math.exp(2 * log_decay))
    )
    fill = jnp.ones((16, width), BF16)

    nets, hazs = (net0_ref, net1_ref, net2_ref, net3_ref), (haz0_ref, haz1_ref, haz2_ref, haz3_ref)

    def prepare(i, slot):
        state = jnp.concatenate([st_ref[i * per_tile + q] for q in range(per_tile)], axis=1)
        rate, hazard = state[0:1], state[5:6]
        ab = ab_ref[i]
        hazs[slot][...] = hazard + ab[:dates] + rate * (ab[dates:] + rate * squares)
        for half in range(2):
            spots = []
            for j in range(ccys):
                at = half * 32 + j * 8
                spots.append(jnp.exp2(log_ref[i, at : at + 8] + state[1 + j : 2 + j]))
            high, mid = split2(jnp.concatenate(spots, axis=0))
            right = jnp.concatenate([high, high, high, mid, mid, fill], axis=0)
            nets[slot][half] = jnp.dot(lhs_ref[half], right, preferred_element_type=F32)

    def weigh(tiles):
        for g in range(0, cps, CROWD):
            scale = ns_ref[0, g : g + CROWD]
            before = []
            for i, slot in tiles:
                for q in range(width // 128):
                    before.append(jnp.exp2(scale * st_ref[i * per_tile + q, 5:6]))
            for t in range(dates):
                at = (t % 8) * cps + g
                total = None
                n = 0
                for i, slot in tiles:
                    for q in range(width // 128):
                        lanes = slice(q * 128, (q + 1) * 128)
                        now = jnp.exp2(ns_ref[t, g : g + CROWD] * hazs[slot][t : t + 1, lanes])
                        worth = jnp.maximum(nets[slot][t // 8, at : at + CROWD, lanes], 0.0) * (before[n] - now)
                        before[n] = now
                        n += 1
                        total = worth if total is None else total + worth
                acc_ref[t * cps + g : t * cps + g + CROWD] += total

    def wait2(k):
        with jax.named_scope(f"wait2_{k}"):
            each_core(lambda n: all_of(s1_send.at[k], s2_recv.at[k], k, 6, n).wait_recv())

    wait2(0)
    prepare(0, 0)
    prepare(1, 1)
    with jax.named_scope("weigh"):

        def step(it):
            i = 4 * it
            prepare(i + 2, 2)
            prepare(i + 3, 3)
            weigh([(i, 0), (i + 1, 1)])
            j = jnp.minimum(i + 4, tiles - 2)
            prepare(j, 0)
            prepare(j + 1, 1)
            weigh([(i + 2, 2), (i + 3, 3)])

        begin = 0
        for k in range(1, chunks + 1):
            end = first[k] // per_tile // 4 - (k < chunks)
            even = begin + (end - begin) // 2 * 2
            if even > begin:
                pl.loop(begin, even, unroll=2)(step)
            if even < end:
                step(even)
            begin = end
            if k == 2:
                own(chunks - 1)
            if k < chunks:
                wait2(k)

    turned = jnp.sum(jnp.transpose(acc_ref[...]), axis=0, keepdims=True)
    part_ref[...] = turned * (1.0 / (total_paths * dt))
    parts_rcv[my_path] = part_ref[...]

    def send_part(i):
        to = ((my_path + i) & (n_path - 1))
        return pltpu.make_async_remote_copy(
            src_ref=part_ref,
            dst_ref=parts_rcv.at[my_path],
            send_sem=t_send.at[0],
            recv_sem=t_recv.at[0],
            device_id={"path": to},
            device_id_type=MESH,
        )

    for i in path_order(n_path):
        send_part(i).start()

    def all_parts(ref, n, at, where):
        return pltpu.make_async_remote_copy(
            src_ref=ref.at[pl.ds(0, n - 1)],
            dst_ref=ref.at[pl.ds(0, n - 1)],
            send_sem=t_send.at[at],
            recv_sem=t_recv.at[at],
            device_id=where,
            device_id_type=MESH,
        )

    lane = iota((1, dates * cps), 1)
    at_date = (lane // cps + me * dates).astype(F32)
    discount = (LOSS_SHARE * dt) * jnp.exp(-RATE_DOM * dt * (at_date + 1.0))
    with jax.named_scope("wait_t1"):
        all_parts(parts_rcv, n_path, 0, {"path": my_path}).wait_recv()
    profile = parts_rcv[0]
    for q in range(1, n_path):
        profile = profile + parts_rcv[q]
    terms = profile * discount
    total = terms[:, :128]
    for q in range(1, dates * cps // 128):
        total = total + terms[:, q * 128 : (q + 1) * 128]
    total = total + pltpu.roll(total, 64, 1)
    total = total + pltpu.roll(total, 32, 1)
    cpart_ref[...] = total
    cparts_rcv[me] = total

    def send_cva(core, i):
        to = ((me + i) & (n_tm - 1))
        return pltpu.make_async_remote_copy(
            src_ref=cpart_ref,
            dst_ref=cparts_rcv.at[me],
            send_sem=t_send.at[1],
            recv_sem=t_recv.at[1],
            device_id={"tm": to, "path": far_path + core},
            device_id_type=MESH,
        )

    @pl.when(near == 1)
    def _():
        for i in tm_order(n_tm):
            send_cva(0, i).start()
            send_cva(1, i).start()

    for t in range(dates):
        prof_out[t : t + 1] = profile[:, t * cps : (t + 1) * cps]


    for k in range(chunks):
        each_core(lambda n: all_of(s1_send.at[k], s1_recv.at[0, k], k, 7, n).wait_send())

        @pl.when(near == 1)
        def _():
            all_of(s2_send.at[0, k], s1_recv.at[0, k], k, 6, n_tm).wait_send()
            all_of(s2_send.at[1, k], s1_recv.at[0, k], k, 6, n_tm - 1).wait_send()

    all_parts(parts_rcv, n_path, 0, {"path": my_path}).wait_send()
    with jax.named_scope("wait_t2"):
        all_parts(cparts_rcv, n_tm, 1, {"tm": me}).wait_recv()
    cva = cparts_rcv[0]
    for q in range(1, n_tm):
        cva = cva + cparts_rcv[q]
    cva_out[...] = cva[:, :cps]

    @pl.when(near == 1)
    def _():
        all_parts(cparts_rcv, n_tm, 1, {"tm": me}).wait_send()
        all_parts(cparts_rcv, n_tm, 1, {"tm": me}).wait_send()


def hand_out(profile, cva, profile_out, cva_out, sems):
    copies = [
        pltpu.make_async_copy(profile, profile_out, sems.at[0]),
        pltpu.make_async_copy(cva, cva_out, sems.at[1]),
    ]
    for copy in copies:
        copy.start()
    for copy in copies:
        copy.wait()


def per_device(n_tm, n_path, shock_rate, shock_fx, fx_vol, fx_corr, hazard_scale, *trades):
    dates, paths = shock_rate.shape
    ccys, cps = fx_vol.shape[0], hazard_scale.shape[0]
    geometry = (n_tm, n_path, paths, dates, cps, ccys, dates * n_tm, paths * n_path)
    width = TILE
    tiles, columns, chunks = paths // width, paths // 128, len(SIZES)
    count = trades[0].shape[0]
    vmem = functools.partial(pl.BlockSpec, memory_space=pltpu.VMEM)
    anywhere = functools.partial(pl.BlockSpec, memory_space=pl.ANY)
    sems = pltpu.SemaphoreType.DMA
    profile, cva = pl.pallas_call(
        functools.partial(kernel, geometry),
        out_shape=(
            pltpu.VMEM((dates, cps), F32),
            pltpu.VMEM((1, cps), F32),
        ),
        in_specs=[anywhere()] * 10,
        out_specs=(vmem(), vmem()),
        scratch_shapes=[
            pltpu.VMEM((dates, paths), F32),
            pltpu.VMEM((ccys, dates, paths), F32),
            pltpu.VMEM((tiles, 64, width), F32),
            pltpu.VMEM((tiles, 32, width), F32),
            pltpu.VMEM((columns, 8, 128), F32),
            pltpu.VMEM((2, columns, 8, 128), F32),
            pltpu.VMEM((2, columns, 8, 128), F32),
            pltpu.VMEM((columns, 8, 128), F32),
            pltpu.VMEM((96, 160), BF16),
            pltpu.VMEM((48, 64), BF16),
            pltpu.VMEM((2, 256, 176), BF16),
            pltpu.VMEM((dates, count), F32),
            pltpu.VMEM((dates, count), F32),
            pltpu.VMEM((dates, cps, 128), F32),
            pltpu.VMEM((2, 256, width), F32),
            pltpu.VMEM((2, 256, width), F32),
            pltpu.VMEM((2, 256, width), F32),
            pltpu.VMEM((2, 256, width), F32),
            pltpu.VMEM((dates, width), F32),
            pltpu.VMEM((dates, width), F32),
            pltpu.VMEM((dates, width), F32),
            pltpu.VMEM((dates, width), F32),
            pltpu.VMEM((dates * cps, 128), F32),
            pltpu.VMEM((1, dates * cps), F32),
            pltpu.VMEM((n_path, 1, dates * cps), F32),
            pltpu.VMEM((1, 128), F32),
            pltpu.VMEM((n_tm, 1, 128), F32),
            pltpu.SMEM((ccys,), F32),
            pltpu.SMEM((ccys,), F32),
            pltpu.SMEM((cps,), F32),
            pltpu.VMEM((1, count), jnp.int32),
            pltpu.VMEM((1, count), jnp.int32),
            pltpu.VMEM((1, count), jnp.int32),
            pltpu.VMEM((1, count), F32),
            pltpu.VMEM((1, count), F32),
            sems((2, chunks)),
            sems((8,)),
            sems((chunks,)),
            sems((2, chunks)),
            sems((2, chunks)),
            sems((chunks,)),
            sems((2,)),
            sems((2,)),
        ],
        compiler_params=pltpu.CompilerParams(collective_id=0, has_side_effects=True),
    )(shock_rate, shock_fx, fx_vol, fx_corr, hazard_scale, *(a.reshape(1, count) for a in trades))
    profile, cva = pl.pallas_call(
        hand_out,
        out_shape=(jax.ShapeDtypeStruct((dates, cps), F32), jax.ShapeDtypeStruct((1, cps), F32)),
        in_specs=[vmem(), vmem()],
        out_specs=(anywhere(), anywhere()),
        scratch_shapes=[sems((2,))],
    )(*(pltpu.with_memory_space_constraint(a, pltpu.VMEM) for a in (profile, cva)))
    return profile, cva.reshape(cps)


def solution(mesh):
    placed = (P("tm", "path"), P(None, "tm", "path"), P(), P(), P(), P(), P(), P(), P(), P())
    return jax.shard_map(
        functools.partial(per_device, mesh.shape["tm"], mesh.shape["path"]),
        mesh=mesh,
        in_specs=placed,
        out_specs=(P("tm", None), P()),
        check_vma=False,
    )
```
